32 devices in a mesh: gx: 2 (over y), gy: 4 (over z), gz: 4 (over x, core).
Axes of the slice: x: 2, y: 2, z: 4, core: 2. Of those that a mesh axis runs over, the one named last changes fastest.
Arguments:
- section: float32 [25, 8, 64, 256], P(None, 'gz', 'gy', 'gx'), may hold values from -0.4 to 1.4, as said below
- base: float32 [25, 8, 64, 256], P(None, 'gz', 'gy', 'gx'), may hold values from -0.4 to 1.4, as said below
- accum: float32 [25, 8, 64, 256], P(None, 'gz', 'gy', 'gx'), may hold values from -4 to 4
Outputs:
- next_section: float32 [25, 8, 64, 256], P(None, 'gz', 'gy', 'gx')
- next_accum: float32 [25, 8, 64, 256], P(None, 'gz', 'gy', 'gx')
- slab: float32 [25, 8, 64, 256], P(None, 'gz')
The draws below stay inside these ranges and needn't reach their ends.
Inputs may be any that keep to these rules, and one draw needn't show every extreme that they name: `section`: fields 0 and 17 (conformal factor and lapse) lie in 0.6 to 1.4; fields 1, 4 and 6 (the metric's diagonal) lie within 0.4 of 1; all other fields lie within 0.4 of 0. `base`: fields 0 and 17 (conformal factor and lapse) lie in 0.6 to 1.4; fields 1, 4 and 6 (the metric's diagonal) lie within 0.4 of 1; all other fields lie within 0.4 of 0.
All inputs are finite; a program needn't handle non-finite values.
Results may differ from the reference program's by a relative error of at most 0.0003.
Values sent between devices are 32-bit elements; how exact they have to be, the bound alone decides.
A program may use at most 64 MiB of HBM per device.

```python
import jax
import jax.numpy as jnp
from jax import lax

FIELDS = 25
CZ = 2
NZ = 8
NY = 64
NX = 256
N_GZ = 4


def draw_fields(key):
    subkeys = jax.random.split(key, 2)
    full_shape = (FIELDS, NZ, NY, NX)
    jitter = jnp.clip(0.1 * jax.random.normal(subkeys[0], full_shape, jnp.float32), -0.4, 0.4)
    positive = 1.0 + jnp.clip(0.15 * jax.random.normal(subkeys[1], full_shape, jnp.float32), -0.4, 0.4)
    field_slot = lax.broadcasted_iota(jnp.int32, full_shape, 0)
    unit_diag = (field_slot == 1) | (field_slot == 4) | (field_slot == 6)
    kept_positive = (field_slot == 0) | (field_slot == 17)
    values = jnp.where(unit_diag, 1.0 + jitter, jitter)
    return jnp.where(kept_positive, positive, values)


def draw_section(key, part):
    return draw_fields(jax.random.fold_in(key, 11))


def draw_base(key, part):
    return draw_fields(jax.random.fold_in(key, 23))


def shard_levels(key, dims, shards, smallest, high):
    gain, own = 1.0, jax.random.fold_in(key, 6)
    for dim, blocks in shards:
        steps = jnp.exp(jax.random.uniform(jax.random.fold_in(own, dim), (blocks,), jnp.float32, smallest / len(shards), high / len(shards)))
        gain = gain * jnp.repeat(steps, dims[dim] // blocks).reshape([-1 if axis == dim else 1 for axis in range(len(dims))])
    return gain


def centred(rng, shape, spread, reach, pieces=(), held_as=jnp.bfloat16):
    entries = jax.random.normal(rng, shape, jnp.float32) * spread
    if len(pieces) > 0:
        entries = shard_levels(rng, shape, pieces, -0.22, 0.18) * entries
    return jnp.clip(entries, min=-reach, max=reach).astype(held_as)


def setup_inputs(seed: int = 0) -> dict:
    streams_of = jax.random.split(jax.random.key(seed), 4)
    section = draw_section(jax.random.fold_in(streams_of[3], 71), 0)
    base = draw_base(jax.random.fold_in(streams_of[3], 71), 0)
    accum = centred(streams_of[2], (FIELDS, NZ, NY, NX), 0.5, 4.0, ((1, 4), (2, 4), (3, 2)), jnp.float32)
    return dict(section=section, base=base, accum=accum)


STEP_DT = 0.25
SPACING = 1.0
DISSIPATE = 0.1
DRIVER_ETA = 2.0
KAPPA_ONE = 0.1
FIRST_TAPS = (1.0 / 12.0, -8.0 / 12.0, 0.0, 8.0 / 12.0, -1.0 / 12.0)
SECOND_TAPS = (-1.0 / 12.0, 16.0 / 12.0, -30.0 / 12.0, 16.0 / 12.0, -1.0 / 12.0)
FOURTH_TAPS = (1.0, -4.0, 6.0, -4.0, 1.0)
PAIR_SLOT = ((0, 1, 2), (1, 3, 4), (2, 4, 5))
PAIR_LIST = ((0, 0), (0, 1), (0, 2), (1, 1), (1, 2), (2, 2))


def window(padded, shifts):
    interior = (padded.shape[1] - 4, padded.shape[2] - 4, padded.shape[3] - 4)
    corner = (2 + shifts[2], 2 + shifts[1], 2 + shifts[0])
    return padded[:, corner[0]:corner[0] + interior[0], corner[1]:corner[1] + interior[1], corner[2]:corner[2] + interior[2]]


def moved(direction, amount):
    shifts = [0, 0, 0]
    shifts[direction] = amount
    return shifts


def line_sum(padded, direction, weights):
    running = None
    for position in range(5):
        if weights[position] != 0.0:
            weighted = weights[position] * window(padded, moved(direction, position - 2))
            running = weighted if running is None else running + weighted
    return running


def cross_sum(padded, first_dir, second_dir):
    running = None
    for first_pos in range(5):
        for second_pos in range(5):
            factor = FIRST_TAPS[first_pos] * FIRST_TAPS[second_pos]
            if factor != 0.0:
                shifts = [0, 0, 0]
                shifts[first_dir] = first_pos - 2
                shifts[second_dir] = second_pos - 2
                weighted = factor * window(padded, shifts)
                running = weighted if running is None else running + weighted
    return running


def evolve_rate(padded):
    centre = window(padded, (0, 0, 0))
    gradients = [line_sum(padded, direction, FIRST_TAPS) / SPACING for direction in range(3)]
    curves = [line_sum(padded, direction, SECOND_TAPS) / (SPACING * SPACING) for direction in range(3)]
    smoothing = line_sum(padded, 0, FOURTH_TAPS) + line_sum(padded, 1, FOURTH_TAPS) + line_sum(padded, 2, FOURTH_TAPS)
    chosen = jnp.concatenate([padded[0:1], padded[17:21]], axis=0)
    mixed_terms = {}
    for dir_pair in ((0, 1), (0, 2), (1, 2)):
        mixed_terms[dir_pair] = cross_sum(chosen, dir_pair[0], dir_pair[1]) / (SPACING * SPACING)

    def second_of(chosen_slot, field_slot, axis_one, axis_two):
        if axis_one == axis_two:
            return curves[axis_one][field_slot]
        return mixed_terms[(min(axis_one, axis_two), max(axis_one, axis_two))][chosen_slot]

    def metric_of(axis_one, axis_two):
        return centre[1 + PAIR_SLOT[axis_one][axis_two]]

    def traceless_of(axis_one, axis_two):
        return centre[8 + PAIR_SLOT[axis_one][axis_two]]

    def inverse_of(axis_one, axis_two):
        return (2.0 if axis_one == axis_two else 0.0) - metric_of(axis_one, axis_two)

    def advect(field_slot):
        return centre[18] * gradients[0][field_slot] + centre[19] * gradients[1][field_slot] + centre[20] * gradients[2][field_slot]

    conformal = centre[0]
    trace_curv = centre[7]
    lapse_field = centre[17]
    theta_field = centre[24]
    divergence = gradients[0][18] + gradients[1][19] + gradients[2][20]
    lap_conformal = curves[0][0] + curves[1][0] + curves[2][0]
    squares_a = sum(traceless_of(axis_one, axis_two) ** 2 for axis_one in range(3) for axis_two in range(3))

    def lapse_dd(axis_one, axis_two):
        return second_of(1, 17, axis_one, axis_two)

    ricci_table = []
    for axis_one, axis_two in PAIR_LIST:
        field_slot = 1 + PAIR_SLOT[axis_one][axis_two]
        flat_part = curves[0][field_slot] + curves[1][field_slot] + curves[2][field_slot]
        conformal_part = second_of(0, 0, axis_one, axis_two) + (lap_conformal if axis_one == axis_two else 0.0)
        ricci_table.append(-0.5 * flat_part + 0.5 * (gradients[axis_one][14 + axis_two] + gradients[axis_two][14 + axis_one]) + conformal_part / (2.0 * conformal))

    def ricci_of(axis_one, axis_two):
        return ricci_table[PAIR_SLOT[axis_one][axis_two]]

    ricci_scalar = conformal * sum(inverse_of(axis_one, axis_two) * ricci_of(axis_one, axis_two) for axis_one in range(3) for axis_two in range(3))
    lapse_trace = sum(inverse_of(axis_one, axis_two) * lapse_dd(axis_one, axis_two) for axis_one in range(3) for axis_two in range(3))

    rates = [None] * 25
    rates[0] = advect(0) + (2.0 / 3.0) * conformal * (lapse_field * trace_curv - divergence)
    for axis_one, axis_two in PAIR_LIST:
        field_slot = PAIR_SLOT[axis_one][axis_two]
        lie_part = sum(metric_of(axis_one, axis_sum) * gradients[axis_two][18 + axis_sum] + metric_of(axis_two, axis_sum) * gradients[axis_one][18 + axis_sum] for axis_sum in range(3))
        rates[1 + field_slot] = advect(1 + field_slot) - 2.0 * lapse_field * traceless_of(axis_one, axis_two) + lie_part - (2.0 / 3.0) * metric_of(axis_one, axis_two) * divergence
    rates[7] = advect(7) - conformal * lapse_trace + lapse_field * (squares_a + trace_curv * trace_curv / 3.0) + KAPPA_ONE * lapse_field * theta_field

    def source_of(axis_one, axis_two):
        return -lapse_dd(axis_one, axis_two) + lapse_field * ricci_of(axis_one, axis_two)

    trace_part = sum(inverse_of(axis_one, axis_two) * source_of(axis_one, axis_two) for axis_one in range(3) for axis_two in range(3))
    for axis_one, axis_two in PAIR_LIST:
        field_slot = PAIR_SLOT[axis_one][axis_two]
        free_part = source_of(axis_one, axis_two) - metric_of(axis_one, axis_two) * trace_part / 3.0
        product_part = sum(traceless_of(axis_one, axis_sum) * traceless_of(axis_sum, axis_two) for axis_sum in range(3))
        lie_part = sum(traceless_of(axis_one, axis_sum) * gradients[axis_two][18 + axis_sum] + traceless_of(axis_two, axis_sum) * gradients[axis_one][18 + axis_sum] for axis_sum in range(3))
        rates[8 + field_slot] = (advect(8 + field_slot) + conformal * free_part
                                 + lapse_field * (trace_curv * traceless_of(axis_one, axis_two) - 2.0 * product_part)
                                 + lie_part - (2.0 / 3.0) * traceless_of(axis_one, axis_two) * divergence)
    for axis_one in range(3):
        gauge_part = (-2.0 * sum(traceless_of(axis_one, axis_two) * gradients[axis_two][17] for axis_two in range(3))
                      + 2.0 * lapse_field * (-(2.0 / 3.0) * sum(inverse_of(axis_one, axis_two) * gradients[axis_two][7] for axis_two in range(3))
                                             - 1.5 * sum(traceless_of(axis_one, axis_two) * gradients[axis_two][0] for axis_two in range(3)) / conformal)
                      + curves[0][18 + axis_one] + curves[1][18 + axis_one] + curves[2][18 + axis_one]
                      + sum(second_of(2 + axis_two, 18 + axis_two, axis_one, axis_two) for axis_two in range(3)) / 3.0
                      + (2.0 / 3.0) * centre[14 + axis_one] * divergence
                      - sum(centre[14 + axis_two] * gradients[axis_two][18 + axis_one] for axis_two in range(3)))
        rates[14 + axis_one] = advect(14 + axis_one) + gauge_part
        rates[18 + axis_one] = advect(18 + axis_one) + 0.75 * centre[21 + axis_one]
        rates[21 + axis_one] = advect(21 + axis_one) + gauge_part - DRIVER_ETA * centre[21 + axis_one]
    rates[17] = advect(17) - 2.0 * lapse_field * (trace_curv - 2.0 * theta_field)
    rates[24] = (advect(24) + 0.5 * lapse_field * (ricci_scalar + (2.0 / 3.0) * trace_curv * trace_curv - squares_a)
                 - 2.0 * KAPPA_ONE * lapse_field * theta_field)
    return jnp.stack(rates, axis=0) + (-DISSIPATE / 16.0) * smoothing


def reference(section, base, accum):
    padded = jnp.pad(section, ((0, 0), (2, 2), (2, 2), (2, 2)), mode="wrap")

    def one_block(block_index):
        start_plane = (block_index * CZ).astype(jnp.int32)
        piece_block = lax.dynamic_slice_in_dim(padded, start_plane, CZ + 4, 1)
        return evolve_rate(piece_block)

    blocks = lax.map(one_block, jnp.arange(N_GZ, dtype=jnp.int32))
    rates = jnp.moveaxis(blocks, 0, 1).reshape(FIELDS, NZ, NY, NX)
    next_section = base + (0.5 * STEP_DT) * rates
    next_accum = accum + (STEP_DT / 3.0) * rates
    return next_section, next_accum, next_section
```

```python
import functools

import jax
import jax.numpy as jnp
from jax import lax
from jax.experimental import pallas as pl
from jax.experimental.pallas import tpu as pltpu
from jax.sharding import PartitionSpec as P

STEP_DT = 0.25
DISSIPATE = 0.1
DRIVER_ETA = 2.0
KAPPA_ONE = 0.1
PAIR_SLOT = ((0, 1, 2), (1, 3, 4), (2, 4, 5))
PAIR_LIST = ((0, 0), (0, 1), (0, 2), (1, 1), (1, 2), (2, 2))
MESH = pl.DeviceIdType.MESH
MIXED = (0, 17, 18, 19, 20)
MIXED_RUNS = ((0, 1), (17, 4))
PAD = 8


def first_of(m2, m1, p1, p2):
    return (8.0 / 12.0) * (p1 - m1) - (1.0 / 12.0) * (p2 - m2)


def rates_of_plane(plane, rows, lanes, xb, tb, emit):
    lane = lax.broadcasted_iota(jnp.int32, (rows, lanes), 1)
    quad = lane & 3
    edge_one = (lane < 1) | (lane >= lanes - 1)
    edge_two = (lane < 2) | (lane >= lanes - 2)

    def cell(field, dz=0, dy=0):
        return xb[field, plane + 2 + dz, PAD + dy : PAD + dy + rows, :]

    def strip(dz=0, dy=0):
        def side(slot):
            return tb[slot, plane + 2 + dz, PAD + dy : PAD + dy + rows, :]

        if tb.shape[0] == 1:
            return side(0)
        return jnp.where(quad < 2, side(1), side(0))

    def inner(edge):
        return jnp.where(
            quad == 1, pltpu.roll(edge, 1, 1), pltpu.roll(edge, lanes - 1, 1)
        )

    def x_line(field, value, edge, edge_in):
        turn = (lanes - 2 - 4 * field) % lanes
        two = pltpu.roll(edge, turn, 1)
        one = pltpu.roll(edge_in, turn, 1)
        m2 = jnp.where(edge_two & (lane < 64), two, pltpu.roll(value, 2, 1))
        m1 = jnp.where(edge_one & (lane < 64), one, pltpu.roll(value, 1, 1))
        p1 = jnp.where(edge_one & (lane >= 64), one, pltpu.roll(value, lanes - 1, 1))
        p2 = jnp.where(edge_two & (lane >= 64), two, pltpu.roll(value, lanes - 2, 1))
        return m2, m1, p1, p2

    def y_line(read):
        return tuple(read(0, dy) for dy in (-2, -1, 1, 2))

    def z_line(read):
        return tuple(read(dz, 0) for dz in (-2, -1, 1, 2))

    edge = strip()
    edge_in = inner(edge)
    edge_y = first_of(*y_line(strip))
    edge_y_in = inner(edge_y)
    edge_z = first_of(*z_line(strip))
    edge_z_in = inner(edge_z)

    centre, grad, curve, lap, smooth, mixed = {}, {}, {}, {}, {}, {}
    need_lap = (0, 1, 2, 3, 4, 5, 6, 17, 18, 19, 20)
    shift = [cell(18), cell(19), cell(20)]
    advected = {}
    for field in range(25):
        value = cell(field)
        read = functools.partial(cell, field)
        lines = [x_line(field, value, edge, edge_in), y_line(read), z_line(read)]
        near = [m1 + p1 for _, m1, p1, _ in lines]
        far = [m2 + p2 for m2, _, _, p2 in lines]
        near_sum = near[0] + near[1] + near[2]
        far_sum = far[0] + far[1] + far[2]
        smooth = far_sum - 4.0 * near_sum + 18.0 * value
        grads = [first_of(*line) for line in lines]
        centre[field] = value
        grad[field] = grads
        advected[field] = (
            shift[0] * grads[0] + shift[1] * grads[1] + shift[2] * grads[2]
            - (DISSIPATE / 16.0) * smooth
        )
        if field in need_lap:
            lap[field] = (16.0 / 12.0) * near_sum - (1.0 / 12.0) * far_sum - 7.5 * value
        if field in MIXED:
            for axis in range(3):
                if field in (0, 17) or field == 18 + axis:
                    curve[field, axis] = (
                        (16.0 / 12.0) * near[axis] - (1.0 / 12.0) * far[axis] - 2.5 * value
                    )
            if field != 20:
                mixed[field, 0, 1] = first_of(*x_line(field, grads[1], edge_y, edge_y_in))
            if field != 19:
                mixed[field, 0, 2] = first_of(*x_line(field, grads[2], edge_z, edge_z_in))
            if field != 18:
                mixed[field, 1, 2] = first_of(
                    *(
                        first_of(*(cell(field, dz, dy) for dy in (-2, -1, 1, 2)))
                        for dz in (-2, -1, 1, 2)
                    )
                )

    def second(field, one, two):
        if one == two:
            return curve[field, one]
        return mixed[field, min(one, two), max(one, two)]

    def sym(table, one, two):
        return table[PAIR_SLOT[one][two]]

    metric = [centre[1 + k] for k in range(6)]
    traceless = [centre[8 + k] for k in range(6)]
    inverse = [
        (2.0 - metric[k]) if one == two else -metric[k]
        for k, (one, two) in enumerate(PAIR_LIST)
    ]
    count = [1.0 if one == two else 2.0 for one, two in PAIR_LIST]

    def contract(left, right):
        diag = left[0] * right[0] + left[3] * right[3] + left[5] * right[5]
        off = left[1] * right[1] + left[2] * right[2] + left[4] * right[4]
        return diag + 2.0 * off

    chi, trace, lapse, theta = centre[0], centre[7], centre[17], centre[24]
    div = grad[18][0] + grad[19][1] + grad[20][2]
    third_div = (2.0 / 3.0) * div
    squares = contract(traceless, traceless)
    over_chi = 1.0 / chi
    half_over = 0.5 * over_chi
    lapse_dd = [second(17, one, two) for one, two in PAIR_LIST]
    ricci = []
    for k, (one, two) in enumerate(PAIR_LIST):
        conf = second(0, one, two)
        if one == two:
            conf = conf + lap[0]
            grads_g = grad[14 + one][one]
        else:
            grads_g = 0.5 * (grad[14 + two][one] + grad[14 + one][two])
        ricci.append(-0.5 * lap[1 + k] + grads_g + conf * half_over)
    ricci_trace = contract(inverse, ricci)
    lapse_trace = contract(inverse, lapse_dd)
    source_trace = lapse * ricci_trace - lapse_trace

    emit(0, advected[0] + (2.0 / 3.0) * chi * (lapse * trace) - chi * third_div)

    def lie_of(table, one, two):
        total = None
        for k in range(3):
            if one == two:
                term = 2.0 * (sym(table, one, k) * grad[18 + k][one])
            else:
                term = (
                    sym(table, one, k) * grad[18 + k][two]
                    + sym(table, two, k) * grad[18 + k][one]
                )
            total = term if total is None else total + term
        return total

    for k, (one, two) in enumerate(PAIR_LIST):
        emit(
            1 + k,
            advected[1 + k]
            - 2.0 * lapse * traceless[k]
            + lie_of(metric, one, two)
            - metric[k] * third_div,
        )
    emit(
        7,
        advected[7]
        - chi * lapse_trace
        + lapse * (squares + trace * trace * (1.0 / 3.0))
        + KAPPA_ONE * lapse * theta,
    )
    third_trace = source_trace * (1.0 / 3.0)
    for k, (one, two) in enumerate(PAIR_LIST):
        free = lapse * ricci[k] - lapse_dd[k] - metric[k] * third_trace
        product = sum(
            sym(traceless, one, m) * sym(traceless, m, two) for m in range(3)
        )
        emit(
            8 + k,
            advected[8 + k]
            + chi * free
            + lapse * (trace * traceless[k] - 2.0 * product)
            + lie_of(traceless, one, two)
            - traceless[k] * third_div,
        )
    gauges = []
    for one in range(3):
        a_lapse = sum(sym(traceless, one, k) * grad[17][k] for k in range(3))
        a_chi = sum(sym(traceless, one, k) * grad[0][k] for k in range(3))
        g_trace = sum(sym(inverse, one, k) * grad[7][k] for k in range(3))
        b_mixed = sum(second(18 + k, one, k) for k in range(3))
        g_shift = sum(centre[14 + k] * grad[18 + one][k] for k in range(3))
        gauge = (
            -2.0 * a_lapse
            - lapse * ((4.0 / 3.0) * g_trace + 3.0 * (a_chi * over_chi))
            + lap[18 + one]
            + b_mixed * (1.0 / 3.0)
            + centre[14 + one] * third_div
            - g_shift
        )
        gauges.append(gauge)
        emit(14 + one, advected[14 + one] + gauge)
    emit(17, advected[17] - 2.0 * lapse * (trace - 2.0 * theta))
    for one in range(3):
        emit(18 + one, advected[18 + one] + 0.75 * centre[21 + one])
    for one in range(3):
        emit(21 + one, advected[21 + one] + gauges[one] - DRIVER_ETA * centre[21 + one])
    emit(
        24,
        advected[24]
        + 0.5 * lapse * (chi * ricci_trace + (2.0 / 3.0) * trace * trace - squares)
        - 2.0 * KAPPA_ONE * lapse * theta,
    )


def section_kernel(
    sizes, groups, section, base, accum, ns_out, na_out, slab_out,
    xb, tb, tile, slab, bb, ab, local_sem, halo_send, halo_recv,
    line_send, gather_recv, out_sem,
):
    gx, gy, gz = sizes
    fields, planes, rows, lanes = section.shape
    i, j, k = (lax.axis_index(name) for name in ("gx", "gy", "gz"))
    group = fields // groups

    def device(dx=0, dy=0, dz=0):
        return (
            lax.rem(i + dx + gx, gx),
            lax.rem(j + dy + gy, gy),
            lax.rem(k + dz + gz, gz),
        )

    x_steps = (1,) if gx == 2 else (1, -1)
    messages = []

    def plane_pair(dz):
        if dz == 0:
            return slice(0, planes), slice(2, 2 + planes)
        if dz == 1:
            return slice(planes - 2, planes), slice(0, 2)
        return slice(0, 2), slice(2 + planes, 4 + planes)

    def row_pair(dy):
        if dy == 0:
            return slice(0, rows), slice(PAD, PAD + rows)
        if dy == 1:
            return slice(rows - PAD, rows), slice(0, PAD)
        return slice(0, PAD), slice(PAD + rows, 2 * PAD + rows)

    def at(ref, lead, plane_cut, row_cut):
        def ds(cut):
            return pl.ds(cut.start, cut.stop - cut.start)

        return ref.at[lead, ds(plane_cut), ds(row_cut), :]

    for dz in (1, -1):
        src_p, dst_p = plane_pair(dz)
        src_r, dst_r = row_pair(0)
        whole = pl.ds(0, fields)
        messages.append(((0, 0, dz), at(section, whole, src_p, src_r), at(xb, whole, dst_p, dst_r)))
    for dy in (1, -1):
        src_p, dst_p = plane_pair(0)
        src_r, dst_r = row_pair(dy)
        messages.append(((0, dy, 0), at(section, whole, src_p, src_r), at(xb, whole, dst_p, dst_r)))
    for dy in (1, -1):
        for dz in (1, -1):
            src_p, dst_p = plane_pair(dz)
            src_r, dst_r = row_pair(dy)
            for start, size in MIXED_RUNS:
                run = pl.ds(start, size)
                messages.append(((0, dy, dz), at(section, run, src_p, src_r), at(xb, run, dst_p, dst_r)))
    direct = len(messages)
    for slot, dx in enumerate(x_steps):
        for dy, dz in ((0, 0), (1, 0), (-1, 0), (0, 1), (0, -1)):
            src_p, dst_p = plane_pair(dz)
            src_r, dst_r = row_pair(dy)
            messages.append(((dx, dy, dz), at(tile, 0, src_p, src_r), at(tb, slot, dst_p, dst_r)))

    load_section = pltpu.make_async_copy(
        section,
        xb.at[:, pl.ds(2, planes), pl.ds(PAD, rows), :],
        local_sem.at[0],
    )
    load_base = pltpu.make_async_copy(base, bb, local_sem.at[1])
    load_accum = pltpu.make_async_copy(accum, ab, local_sem.at[2])
    load_section.start()

    partners = []
    for delta, _, _ in messages:
        if delta not in partners:
            partners.append(delta)
    barrier = pltpu.get_barrier_semaphore()
    for delta in partners:
        pl.semaphore_signal(barrier, inc=1, device_id=device(*delta), device_id_type=MESH)
    pl.semaphore_wait(barrier, len(partners))

    copies = [
        pltpu.make_async_remote_copy(
            src_ref=src, dst_ref=dst, send_sem=halo_send.at[m], recv_sem=halo_recv.at[m],
            device_id=device(*delta), device_id_type=MESH,
        )
        for m, (delta, src, dst) in enumerate(messages)
    ]
    load_section.wait()
    lane = lax.broadcasted_iota(jnp.int32, (rows, lanes), 1)

    def pack(plane, carry):
        packed = jnp.zeros((rows, lanes), jnp.float32)
        for field in range(fields):
            value = xb[field, plane + 2, PAD : PAD + rows, :]
            ends = jnp.where(lane < 2, value, pltpu.roll(value, 4, 1))
            if field:
                ends = pltpu.roll(ends, 4 * field, 1)
            packed = jnp.where((lane >> 2) == field, ends, packed)
        tile[0, plane] = packed
        return carry

    lax.fori_loop(0, planes, pack, 0)
    for copy in copies[:direct]:
        copy.start()
    for copy in copies[direct:]:
        copy.start()
    load_base.start()
    load_accum.start()
    load_base.wait()
    load_accum.wait()
    for copy in copies:
        copy.wait_recv()

    own_rows = pl.ds(pl.multiple_of(j * rows, rows), rows)
    own_cols = pl.ds(pl.multiple_of(i * lanes, lanes), lanes)

    def step(plane, carry):
        def emit(field, rate):
            slab[field, plane, own_rows, own_cols] = bb[field, plane] + (0.5 * STEP_DT) * rate
            ab[field, plane] = ab[field, plane] + (STEP_DT / 3.0) * rate

        rates_of_plane(plane, rows, lanes, xb, tb, emit)
        return carry

    lax.fori_loop(0, planes, step, 0)

    def piece(ref, bi, bj, c=None):
        lead = pl.ds(0, fields) if c is None else pl.ds(c * group, group)
        return ref.at[
            lead,
            :,
            pl.ds(pl.multiple_of(bj * rows, rows), rows),
            pl.ds(pl.multiple_of(bi * lanes, lanes), lanes),
        ]

    towards = ((0, 1), (0, -1), (1, 0), (-1, 0))

    def send(link, bi, bj, c):
        dx, dy = towards[link]
        return pltpu.make_async_remote_copy(
            src_ref=piece(slab, bi, bj, c),
            dst_ref=piece(slab, bi, bj, c),
            send_sem=line_send.at[link, bi, bj, c],
            recv_sem=gather_recv.at[bi, bj, c],
            device_id=device(dx, dy, 0),
            device_id_type=MESH,
        )

    def arrive(bi, bj, c):
        part = piece(slab, bi, bj, c)
        pltpu.make_async_remote_copy(
            src_ref=part, dst_ref=part, send_sem=line_send.at[0, bi, bj, c],
            recv_sem=gather_recv.at[bi, bj, c], device_id=device(0, 1, 0),
            device_id_type=MESH,
        ).wait_recv()

    def to_hbm(bi, bj):
        return pltpu.make_async_copy(
            piece(slab, bi, bj), piece(slab_out, bi, bj), out_sem.at[bi, bj]
        )

    paired = gx == 2 and gy % 2 == 0
    turned = (groups * 2) // 5 if paired else 0
    pair = j + 1 - 2 * lax.rem(j, 2)

    def each(count, body, start=0):
        lax.fori_loop(start, count, lambda c, carry: (body(c), carry)[1], 0)

    def x_links(body):
        @pl.when(i + 1 < gx)
        def _():
            body(2)

        @pl.when(i > 0)
        def _():
            body(3)

    def own(c):
        @pl.when(j + 1 < gy)
        def _():
            send(0, i, j, c).start()

        @pl.when(j > 0)
        def _():
            send(1, i, j, c).start()

        x_links(lambda link: send(link, i, j, c).start())

    each(groups, own)
    to_hbm(i, j).start()
    ns_copy = pltpu.make_async_copy(piece(slab, i, j), ns_out, local_sem.at[0])
    na_copy = pltpu.make_async_copy(ab, na_out, local_sem.at[1])
    ns_copy.start()
    na_copy.start()

    def crossed(d, bj, c, body):
        if d == 1 and turned:
            @pl.when((bj != pair) | (c >= turned))
            def _():
                body()
        else:
            body()

    other = 1 - i

    for d in range(1, gy):
        def column(c, d=d):
            @pl.when(j - d >= 0)
            def _():
                bj = j - d
                arrive(i, bj, c)

                @pl.when(j + 1 < gy)
                def _():
                    send(0, i, bj, c).start()

                crossed(d, bj, c, lambda: x_links(lambda link: send(link, i, bj, c).start()))

            @pl.when(j + d < gy)
            def _():
                bj = j + d
                arrive(i, bj, c)

                @pl.when(j > 0)
                def _():
                    send(1, i, bj, c).start()

                crossed(d, bj, c, lambda: x_links(lambda link: send(link, i, bj, c).start()))

            if d == 1 and turned:
                @pl.when(c < turned)
                def _():
                    arrive(other, j, c)

                    @pl.when(pair > j)
                    def _():
                        send(0, other, j, c).start()

                    @pl.when(pair < j)
                    def _():
                        send(1, other, j, c).start()

        each(groups, column)

        @pl.when(j - d >= 0)
        def _():
            to_hbm(i, j - d).start()

        @pl.when(j + d < gy)
        def _():
            to_hbm(i, j + d).start()

    def block_rows(body):
        body(j, True)
        for d in range(1, gy):
            @pl.when(j - d >= 0)
            def _():
                body(j - d, False)

            @pl.when(j + d < gy)
            def _():
                body(j + d, False)

    for d in range(1, gx):
        def row(bj, first, d=d):
            @pl.when(i - d >= 0)
            def _():
                def take(c):
                    arrive(i - d, bj, c)

                    @pl.when(i + 1 < gx)
                    def _():
                        send(2, i - d, bj, c).start()

                each(groups, take, turned if first else 0)
                to_hbm(i - d, bj).start()

            @pl.when(i + d < gx)
            def _():
                def take(c):
                    arrive(i + d, bj, c)

                    @pl.when(i > 0)
                    def _():
                        send(3, i + d, bj, c).start()

                each(groups, take, turned if first else 0)
                to_hbm(i + d, bj).start()

        block_rows(row)

    for copy in copies:
        copy.wait_send()

    def drain(bj):
        def chunk(c):
            @pl.when((bj <= j) & (j + 1 < gy))
            def _():
                send(0, i, bj, c).wait_send()

            @pl.when((bj >= j) & (j > 0))
            def _():
                send(1, i, bj, c).wait_send()

            def sideways(link):
                send(link, i, bj, c).wait_send()

            if turned:
                @pl.when((bj != pair) | (c >= turned))
                def _():
                    x_links(sideways)
            else:
                x_links(sideways)

            for d in range(1, gx):
                @pl.when((i - d >= 0) & (i + 1 < gx))
                def _():
                    send(2, i - d, bj, c).wait_send()

                @pl.when((i + d < gx) & (i > 0))
                def _():
                    send(3, i + d, bj, c).wait_send()

        each(groups, chunk)

    each(gy, drain)
    if turned:
        def drain_turned(c):
            @pl.when(pair > j)
            def _():
                send(0, other, j, c).wait_send()

            @pl.when(pair < j)
            def _():
                send(1, other, j, c).wait_send()

        each(turned, drain_turned)
    for bi in range(gx):
        each(gy, lambda bj, bi=bi: to_hbm(bi, bj).wait())
    ns_copy.wait()
    na_copy.wait()


def shards(sizes, section, base, accum):
    gx, gy, gz = sizes
    fields, planes, rows, lanes = section.shape
    groups = 5
    slots = 1 if gx == 2 else 2
    n_messages = 4 + 4 * len(MIXED_RUNS) + 5 * slots
    any_spec = pl.BlockSpec(memory_space=pl.ANY)
    block = jax.ShapeDtypeStruct(section.shape, jnp.float32)
    slab = jax.ShapeDtypeStruct((fields, planes, gy * rows, gx * lanes), jnp.float32)
    dma = pltpu.SemaphoreType.DMA
    return pl.pallas_call(
        functools.partial(section_kernel, sizes, groups),
        out_shape=(block, block, slab),
        in_specs=[any_spec] * 3,
        out_specs=(any_spec,) * 3,
        scratch_shapes=[
            pltpu.VMEM((fields, planes + 4, rows + 2 * PAD, lanes), jnp.float32),
            pltpu.VMEM((slots, planes + 4, rows + 2 * PAD, lanes), jnp.float32),
            pltpu.VMEM((1, planes, rows, lanes), jnp.float32),
            pltpu.VMEM(slab.shape, jnp.float32),
            pltpu.VMEM(section.shape, jnp.float32),
            pltpu.VMEM(section.shape, jnp.float32),
            dma((3,)),
            dma((n_messages,)),
            dma((n_messages,)),
            dma((4, gx, gy, groups)),
            dma((gx, gy, groups)),
            dma((gx, gy)),
        ],
        compiler_params=pltpu.CompilerParams(collective_id=0, has_side_effects=True),
    )(section, base, accum)


def solution(mesh):
    sizes = tuple(mesh.shape[name] for name in ("gx", "gy", "gz"))
    spec = P(None, "gz", "gy", "gx")
    return jax.shard_map(
        functools.partial(shards, sizes),
        mesh=mesh,
        in_specs=(spec, spec, spec),
        out_specs=(spec, spec, P(None, "gz", None, None)),
        check_vma=False,
    )
```

```python
import functools

import jax
import jax.numpy as jnp
from jax import lax
from jax.experimental import pallas as pl
from jax.experimental.pallas import tpu as pltpu
from jax.sharding import PartitionSpec as P

STEP_DT = 0.25
DISSIPATE = 0.1
DRIVER_ETA = 2.0
KAPPA_ONE = 0.1
PAIR_SLOT = ((0, 1, 2), (1, 3, 4), (2, 4, 5))
PAIR_LIST = ((0, 0), (0, 1), (0, 2), (1, 1), (1, 2), (2, 2))
MESH = pl.DeviceIdType.MESH
MIXED = (0, 17, 18, 19, 20)
MIXED_RUNS = ((0, 1), (17, 4))
PAD = 8


def first_of(m2, m1, p1, p2):
    return (8.0 / 12.0) * (p1 - m1) - (1.0 / 12.0) * (p2 - m2)


def rates_of_plane(plane, rows, lanes, xb, tb, emit):
    lane = lax.broadcasted_iota(jnp.int32, (rows, lanes), 1)
    quad = lane & 3
    edge_one = (lane < 1) | (lane >= lanes - 1)
    edge_two = (lane < 2) | (lane >= lanes - 2)

    def cell(field, dz=0, dy=0):
        return xb[field, plane + 2 + dz, PAD + dy : PAD + dy + rows, :]

    def strip(dz=0, dy=0):
        def side(slot):
            return tb[slot, plane + 2 + dz, PAD + dy : PAD + dy + rows, :]

        if tb.shape[0] == 1:
            return side(0)
        return jnp.where(quad < 2, side(1), side(0))

    def inner(edge):
        return jnp.where(
            quad == 1, pltpu.roll(edge, 1, 1), pltpu.roll(edge, lanes - 1, 1)
        )

    def x_line(field, value, edge, edge_in):
        turn = (lanes - 2 - 4 * field) % lanes
        two = pltpu.roll(edge, turn, 1)
        one = pltpu.roll(edge_in, turn, 1)
        m2 = jnp.where(edge_two & (lane < 64), two, pltpu.roll(value, 2, 1))
        m1 = jnp.where(edge_one & (lane < 64), one, pltpu.roll(value, 1, 1))
        p1 = jnp.where(edge_one & (lane >= 64), one, pltpu.roll(value, lanes - 1, 1))
        p2 = jnp.where(edge_two & (lane >= 64), two, pltpu.roll(value, lanes - 2, 1))
        return m2, m1, p1, p2

    def y_line(read):
        return tuple(read(0, dy) for dy in (-2, -1, 1, 2))

    def z_line(read):
        return tuple(read(dz, 0) for dz in (-2, -1, 1, 2))

    edge = strip()
    edge_in = inner(edge)
    edge_y = first_of(*y_line(strip))
    edge_y_in = inner(edge_y)
    edge_z = first_of(*z_line(strip))
    edge_z_in = inner(edge_z)

    centre, grad, curve, lap, smooth, mixed = {}, {}, {}, {}, {}, {}
    need_lap = (0, 1, 2, 3, 4, 5, 6, 17, 18, 19, 20)
    shift = [cell(18), cell(19), cell(20)]
    advected = {}
    for field in range(25):
        value = cell(field)
        read = functools.partial(cell, field)
        lines = [x_line(field, value, edge, edge_in), y_line(read), z_line(read)]
        near = [m1 + p1 for _, m1, p1, _ in lines]
        far = [m2 + p2 for m2, _, _, p2 in lines]
        near_sum = near[0] + near[1] + near[2]
        far_sum = far[0] + far[1] + far[2]
        smooth = far_sum - 4.0 * near_sum + 18.0 * value
        grads = [first_of(*line) for line in lines]
        centre[field] = value
        grad[field] = grads
        advected[field] = (
            shift[0] * grads[0] + shift[1] * grads[1] + shift[2] * grads[2]
            - (DISSIPATE / 16.0) * smooth
        )
        if field in need_lap:
            lap[field] = (16.0 / 12.0) * near_sum - (1.0 / 12.0) * far_sum - 7.5 * value
        if field in MIXED:
            for axis in range(3):
                if field in (0, 17) or field == 18 + axis:
                    curve[field, axis] = (
                        (16.0 / 12.0) * near[axis] - (1.0 / 12.0) * far[axis] - 2.5 * value
                    )
            if field != 20:
                mixed[field, 0, 1] = first_of(*x_line(field, grads[1], edge_y, edge_y_in))
            if field != 19:
                mixed[field, 0, 2] = first_of(*x_line(field, grads[2], edge_z, edge_z_in))
            if field != 18:
                mixed[field, 1, 2] = first_of(
                    *(
                        first_of(*(cell(field, dz, dy) for dy in (-2, -1, 1, 2)))
                        for dz in (-2, -1, 1, 2)
                    )
                )

    def second(field, one, two):
        if one == two:
            return curve[field, one]
        return mixed[field, min(one, two), max(one, two)]

    def sym(table, one, two):
        return table[PAIR_SLOT[one][two]]

    metric = [centre[1 + k] for k in range(6)]
    traceless = [centre[8 + k] for k in range(6)]
    inverse = [
        (2.0 - metric[k]) if one == two else -metric[k]
        for k, (one, two) in enumerate(PAIR_LIST)
    ]
    count = [1.0 if one == two else 2.0 for one, two in PAIR_LIST]

    def contract(left, right):
        diag = left[0] * right[0] + left[3] * right[3] + left[5] * right[5]
        off = left[1] * right[1] + left[2] * right[2] + left[4] * right[4]
        return diag + 2.0 * off

    chi, trace, lapse, theta = centre[0], centre[7], centre[17], centre[24]
    div = grad[18][0] + grad[19][1] + grad[20][2]
    third_div = (2.0 / 3.0) * div
    squares = contract(traceless, traceless)
    over_chi = 1.0 / chi
    half_over = 0.5 * over_chi
    lapse_dd = [second(17, one, two) for one, two in PAIR_LIST]
    ricci = []
    for k, (one, two) in enumerate(PAIR_LIST):
        conf = second(0, one, two)
        if one == two:
            conf = conf + lap[0]
            grads_g = grad[14 + one][one]
        else:
            grads_g = 0.5 * (grad[14 + two][one] + grad[14 + one][two])
        ricci.append(-0.5 * lap[1 + k] + grads_g + conf * half_over)
    ricci_trace = contract(inverse, ricci)
    lapse_trace = contract(inverse, lapse_dd)
    source_trace = lapse * ricci_trace - lapse_trace

    emit(0, advected[0] + (2.0 / 3.0) * chi * (lapse * trace) - chi * third_div)

    def lie_of(table, one, two):
        total = None
        for k in range(3):
            if one == two:
                term = 2.0 * (sym(table, one, k) * grad[18 + k][one])
            else:
                term = (
                    sym(table, one, k) * grad[18 + k][two]
                    + sym(table, two, k) * grad[18 + k][one]
                )
            total = term if total is None else total + term
        return total

    for k, (one, two) in enumerate(PAIR_LIST):
        emit(
            1 + k,
            advected[1 + k]
            - 2.0 * lapse * traceless[k]
            + lie_of(metric, one, two)
            - metric[k] * third_div,
        )
    emit(
        7,
        advected[7]
        - chi * lapse_trace
        + lapse * (squares + trace * trace * (1.0 / 3.0))
        + KAPPA_ONE * lapse * theta,
    )
    third_trace = source_trace * (1.0 / 3.0)
    for k, (one, two) in enumerate(PAIR_LIST):
        free = lapse * ricci[k] - lapse_dd[k] - metric[k] * third_trace
        product = sum(
            sym(traceless, one, m) * sym(traceless, m, two) for m in range(3)
        )
        emit(
            8 + k,
            advected[8 + k]
            + chi * free
            + lapse * (trace * traceless[k] - 2.0 * product)
            + lie_of(traceless, one, two)
            - traceless[k] * third_div,
        )
    gauges = []
    for one in range(3):
        a_lapse = sum(sym(traceless, one, k) * grad[17][k] for k in range(3))
        a_chi = sum(sym(traceless, one, k) * grad[0][k] for k in range(3))
        g_trace = sum(sym(inverse, one, k) * grad[7][k] for k in range(3))
        b_mixed = sum(second(18 + k, one, k) for k in range(3))
        g_shift = sum(centre[14 + k] * grad[18 + one][k] for k in range(3))
        gauge = (
            -2.0 * a_lapse
            - lapse * ((4.0 / 3.0) * g_trace + 3.0 * (a_chi * over_chi))
            + lap[18 + one]
            + b_mixed * (1.0 / 3.0)
            + centre[14 + one] * third_div
            - g_shift
        )
        gauges.append(gauge)
        emit(14 + one, advected[14 + one] + gauge)
    emit(17, advected[17] - 2.0 * lapse * (trace - 2.0 * theta))
    for one in range(3):
        emit(18 + one, advected[18 + one] + 0.75 * centre[21 + one])
    for one in range(3):
        emit(21 + one, advected[21 + one] + gauges[one] - DRIVER_ETA * centre[21 + one])
    emit(
        24,
        advected[24]
        + 0.5 * lapse * (chi * ricci_trace + (2.0 / 3.0) * trace * trace - squares)
        - 2.0 * KAPPA_ONE * lapse * theta,
    )


def section_kernel(
    sizes, groups, section, base, accum, ns_out, na_out, slab,
    xb, tb, tile, bb, ab, local_sem, halo_send, halo_recv,
    line_send, gather_recv,
):
    gx, gy, gz = sizes
    fields, planes, rows, lanes = section.shape
    i, j, k = (lax.axis_index(name) for name in ("gx", "gy", "gz"))
    group = fields // groups

    def device(dx=0, dy=0, dz=0):
        return (
            lax.rem(i + dx + gx, gx),
            lax.rem(j + dy + gy, gy),
            lax.rem(k + dz + gz, gz),
        )

    x_steps = (1,) if gx == 2 else (1, -1)
    messages = []

    def plane_pair(dz):
        if dz == 0:
            return slice(0, planes), slice(2, 2 + planes)
        if dz == 1:
            return slice(planes - 2, planes), slice(0, 2)
        return slice(0, 2), slice(2 + planes, 4 + planes)

    def row_pair(dy):
        if dy == 0:
            return slice(0, rows), slice(PAD, PAD + rows)
        if dy == 1:
            return slice(rows - 2, rows), slice(PAD - 2, PAD)
        return slice(0, 2), slice(PAD + rows, PAD + rows + 2)

    def at(ref, lead, plane_cut, row_cut):
        def ds(cut):
            return pl.ds(cut.start, cut.stop - cut.start)

        return ref.at[lead, ds(plane_cut), ds(row_cut), :]

    for dz in (1, -1):
        src_p, dst_p = plane_pair(dz)
        src_r, dst_r = row_pair(0)
        whole = pl.ds(0, fields)
        messages.append(((0, 0, dz), at(section, whole, src_p, src_r), at(xb, whole, dst_p, dst_r)))
    for dy in (1, -1):
        src_p, dst_p = plane_pair(0)
        src_r, dst_r = row_pair(dy)
        messages.append(((0, dy, 0), at(section, whole, src_p, src_r), at(xb, whole, dst_p, dst_r)))
    for dy in (1, -1):
        for dz in (1, -1):
            src_p, dst_p = plane_pair(dz)
            src_r, dst_r = row_pair(dy)
            for start, size in MIXED_RUNS:
                run = pl.ds(start, size)
                messages.append(((0, dy, dz), at(section, run, src_p, src_r), at(xb, run, dst_p, dst_r)))
    direct = len(messages)
    for slot, dx in enumerate(x_steps):
        for dy, dz in ((0, 0), (1, 0), (-1, 0), (0, 1), (0, -1)):
            src_p, dst_p = plane_pair(dz)
            src_r, dst_r = row_pair(dy)
            messages.append(((dx, dy, dz), at(tile, 0, src_p, src_r), at(tb, slot, dst_p, dst_r)))

    load_section = pltpu.make_async_copy(
        section,
        xb.at[:, pl.ds(2, planes), pl.ds(PAD, rows), :],
        local_sem.at[0],
    )
    load_base = pltpu.make_async_copy(base, bb, local_sem.at[1])
    load_accum = pltpu.make_async_copy(accum, ab, local_sem.at[2])
    load_section.start()

    partners = []
    for delta, _, _ in messages:
        if delta not in partners:
            partners.append(delta)
    barrier = pltpu.get_barrier_semaphore()
    for delta in partners:
        pl.semaphore_signal(barrier, inc=1, device_id=device(*delta), device_id_type=MESH)
    pl.semaphore_wait(barrier, len(partners))

    copies = [
        pltpu.make_async_remote_copy(
            src_ref=src, dst_ref=dst, send_sem=halo_send.at[m], recv_sem=halo_recv.at[m],
            device_id=device(*delta), device_id_type=MESH,
        )
        for m, (delta, src, dst) in enumerate(messages)
    ]
    load_section.wait()
    lane = lax.broadcasted_iota(jnp.int32, (rows, lanes), 1)

    def pack(plane, carry):
        packed = jnp.zeros((rows, lanes), jnp.float32)
        for field in range(fields):
            value = xb[field, plane + 2, PAD : PAD + rows, :]
            ends = jnp.where(lane < 2, value, pltpu.roll(value, 4, 1))
            if field:
                ends = pltpu.roll(ends, 4 * field, 1)
            packed = jnp.where((lane >> 2) == field, ends, packed)
        tile[0, plane] = packed
        return carry

    lax.fori_loop(0, planes, pack, 0)
    for copy in copies[:direct]:
        copy.start()
    for copy in copies[direct:]:
        copy.start()
    load_base.start()
    load_accum.start()
    load_base.wait()
    load_accum.wait()
    for copy in copies:
        copy.wait_recv()

    own_rows = pl.ds(pl.multiple_of(j * rows, rows), rows)
    own_cols = pl.ds(pl.multiple_of(i * lanes, lanes), lanes)

    def step(plane, carry):
        def emit(field, rate):
            slab[field, plane, own_rows, own_cols] = bb[field, plane] + (0.5 * STEP_DT) * rate
            ns_out[field, plane] = bb[field, plane] + (0.5 * STEP_DT) * rate
            na_out[field, plane] = ab[field, plane] + (STEP_DT / 3.0) * rate

        rates_of_plane(plane, rows, lanes, xb, tb, emit)
        return carry

    lax.fori_loop(0, planes, step, 0)

    def piece(ref, bi, bj, c=None):
        lead = pl.ds(0, fields) if c is None else pl.ds(c * group, group)
        return ref.at[
            lead,
            :,
            pl.ds(pl.multiple_of(bj * rows, rows), rows),
            pl.ds(pl.multiple_of(bi * lanes, lanes), lanes),
        ]

    towards = ((0, 1), (0, -1), (1, 0), (-1, 0))

    def send(link, bi, bj, c):
        dx, dy = towards[link]
        return pltpu.make_async_remote_copy(
            src_ref=piece(slab, bi, bj, c),
            dst_ref=piece(slab, bi, bj, c),
            send_sem=line_send.at[link, bi, bj, c],
            recv_sem=gather_recv.at[bi, bj, c],
            device_id=device(dx, dy, 0),
            device_id_type=MESH,
        )

    def arrive(bi, bj, c):
        part = piece(slab, bi, bj, c)
        pltpu.make_async_remote_copy(
            src_ref=part, dst_ref=part, send_sem=line_send.at[0, bi, bj, c],
            recv_sem=gather_recv.at[bi, bj, c], device_id=device(0, 1, 0),
            device_id_type=MESH,
        ).wait_recv()

    paired = gx == 2 and gy % 2 == 0
    turned = (groups * 2) // 5 if paired else 0
    pair = j + 1 - 2 * lax.rem(j, 2)

    def each(count, body, start=0):
        lax.fori_loop(start, count, lambda c, carry: (body(c), carry)[1], 0)

    def x_links(body):
        @pl.when(i + 1 < gx)
        def _():
            body(2)

        @pl.when(i > 0)
        def _():
            body(3)

    def own(c):
        @pl.when(j + 1 < gy)
        def _():
            send(0, i, j, c).start()

        @pl.when(j > 0)
        def _():
            send(1, i, j, c).start()

        x_links(lambda link: send(link, i, j, c).start())

    each(groups, own)

    def crossed(d, bj, c, body):
        if d == 1 and turned:
            @pl.when((bj != pair) | (c >= turned))
            def _():
                body()
        else:
            body()

    other = 1 - i

    for d in range(1, gy):
        def column(c, d=d):
            @pl.when(j - d >= 0)
            def _():
                bj = j - d
                arrive(i, bj, c)

                @pl.when(j + 1 < gy)
                def _():
                    send(0, i, bj, c).start()

                crossed(d, bj, c, lambda: x_links(lambda link: send(link, i, bj, c).start()))

            @pl.when(j + d < gy)
            def _():
                bj = j + d
                arrive(i, bj, c)

                @pl.when(j > 0)
                def _():
                    send(1, i, bj, c).start()

                crossed(d, bj, c, lambda: x_links(lambda link: send(link, i, bj, c).start()))

            if d == 1 and turned:
                @pl.when(c < turned)
                def _():
                    arrive(other, j, c)

                    @pl.when(pair > j)
                    def _():
                        send(0, other, j, c).start()

                    @pl.when(pair < j)
                    def _():
                        send(1, other, j, c).start()

        each(groups, column)

        @pl.when(j - d >= 0)
        def _():
            pass

        @pl.when(j + d < gy)
        def _():
            pass

    def block_rows(body):
        body(j, True)
        for d in range(1, gy):
            @pl.when(j - d >= 0)
            def _():
                body(j - d, False)

            @pl.when(j + d < gy)
            def _():
                body(j + d, False)

    for d in range(1, gx):
        def row(bj, first, d=d):
            @pl.when(i - d >= 0)
            def _():
                def take(c):
                    arrive(i - d, bj, c)

                    @pl.when(i + 1 < gx)
                    def _():
                        send(2, i - d, bj, c).start()

                each(groups, take, turned if first else 0)
                pass

            @pl.when(i + d < gx)
            def _():
                def take(c):
                    arrive(i + d, bj, c)

                    @pl.when(i > 0)
                    def _():
                        send(3, i + d, bj, c).start()

                each(groups, take, turned if first else 0)
                pass

        block_rows(row)

    for copy in copies:
        copy.wait_send()

    def drain(bj):
        def chunk(c):
            @pl.when((bj <= j) & (j + 1 < gy))
            def _():
                send(0, i, bj, c).wait_send()

            @pl.when((bj >= j) & (j > 0))
            def _():
                send(1, i, bj, c).wait_send()

            def sideways(link):
                send(link, i, bj, c).wait_send()

            if turned:
                @pl.when((bj != pair) | (c >= turned))
                def _():
                    x_links(sideways)
            else:
                x_links(sideways)

            for d in range(1, gx):
                @pl.when((i - d >= 0) & (i + 1 < gx))
                def _():
                    send(2, i - d, bj, c).wait_send()

                @pl.when((i + d < gx) & (i > 0))
                def _():
                    send(3, i + d, bj, c).wait_send()

        each(groups, chunk)

    each(gy, drain)
    if turned:
        def drain_turned(c):
            @pl.when(pair > j)
            def _():
                send(0, other, j, c).wait_send()

            @pl.when(pair < j)
            def _():
                send(1, other, j, c).wait_send()

        each(turned, drain_turned)


def put_out(ns_in, na_in, slab_in, ns_out, na_out, slab_out, sem):
    pairs = ((slab_in, slab_out), (ns_in, ns_out), (na_in, na_out))
    copies = [pltpu.make_async_copy(a, b, sem.at[n]) for n, (a, b) in enumerate(pairs)]
    for copy in copies:
        copy.start()
    for copy in copies:
        copy.wait()


def shards(sizes, section, base, accum):
    gx, gy, gz = sizes
    fields, planes, rows, lanes = section.shape
    groups = 5
    slots = 1 if gx == 2 else 2
    n_messages = 4 + 4 * len(MIXED_RUNS) + 5 * slots
    any_spec = pl.BlockSpec(memory_space=pl.ANY)
    block = jax.ShapeDtypeStruct(section.shape, jnp.float32)
    slab = jax.ShapeDtypeStruct((fields, planes, gy * rows, gx * lanes), jnp.float32)
    dma = pltpu.SemaphoreType.DMA
    staged = pl.pallas_call(
        functools.partial(section_kernel, sizes, groups),
        out_shape=(block, block, slab),
        in_specs=[pl.BlockSpec(memory_space=pltpu.HBM)] * 3,
        out_specs=(pl.BlockSpec(memory_space=pltpu.VMEM),) * 3,
        scratch_shapes=[
            pltpu.VMEM((fields, planes + 4, rows + 2 * PAD, lanes), jnp.float32),
            pltpu.VMEM((slots, planes + 4, rows + 2 * PAD, lanes), jnp.float32),
            pltpu.VMEM((1, planes, rows, lanes), jnp.float32),
            pltpu.VMEM(section.shape, jnp.float32),
            pltpu.VMEM(section.shape, jnp.float32),
            dma((3,)),
            dma((n_messages,)),
            dma((n_messages,)),
            dma((4, gx, gy, groups)),
            dma((gx, gy, groups)),
        ],
        compiler_params=pltpu.CompilerParams(collective_id=0, has_side_effects=True, vmem_limit_bytes=24 << 20),
    )(section, base, accum)
    return pl.pallas_call(
        put_out,
        out_shape=(block, block, slab),
        in_specs=[pl.BlockSpec(memory_space=pltpu.VMEM)] * 3,
        out_specs=(any_spec,) * 3,
        scratch_shapes=[dma((3,))],
        compiler_params=pltpu.CompilerParams(vmem_limit_bytes=8 << 20),
    )(*staged)


def solution(mesh):
    sizes = tuple(mesh.shape[name] for name in ("gx", "gy", "gz"))
    spec = P(None, "gz", "gy", "gx")
    return jax.shard_map(
        functools.partial(shards, sizes),
        mesh=mesh,
        in_specs=(spec, spec, spec),
        out_specs=(spec, spec, P(None, "gz", None, None)),
        check_vma=False,
    )
```

```python
import functools

import jax
import jax.numpy as jnp
from jax import lax
from jax.experimental import pallas as pl
from jax.experimental.pallas import tpu as pltpu
from jax.sharding import PartitionSpec as P

STEP_DT = 0.25
DISSIPATE = 0.1
DRIVER_ETA = 2.0
KAPPA_ONE = 0.1
PAIR_SLOT = ((0, 1, 2), (1, 3, 4), (2, 4, 5))
PAIR_LIST = ((0, 0), (0, 1), (0, 2), (1, 1), (1, 2), (2, 2))
MESH = pl.DeviceIdType.MESH
MIXED = (0, 17, 18, 19, 20)
RUNS = ((0, 1), (17, 4), (1, 5), (6, 2), (14, 3), (8, 5), (13, 1), (21, 4))
GROUPS = 5
ORDER = tuple(first + n for first, size in RUNS for n in range(size))
PLACE = tuple(ORDER.index(field) for field in range(len(ORDER)))
PAD = 8


def first_of(m2, m1, p1, p2):
    return (8.0 / 12.0) * (p1 - m1) - (1.0 / 12.0) * (p2 - m2)


def rates_of_plane(plane, rows, lanes, xb, tb, emit):
    lane = lax.broadcasted_iota(jnp.int32, (rows, lanes), 1)
    quad = lane & 3
    edge_one = (lane < 1) | (lane >= lanes - 1)
    edge_two = (lane < 2) | (lane >= lanes - 2)

    def cell(field, dz=0, dy=0):
        return xb[PLACE[field], plane + 2 + dz, PAD + dy : PAD + dy + rows, :]

    def strip(dz=0, dy=0):
        def side(slot):
            return tb[slot, plane + 2 + dz, PAD + dy : PAD + dy + rows, :]

        if tb.shape[0] == 1:
            return side(0)
        return jnp.where(quad < 2, side(1), side(0))

    def inner(edge):
        return jnp.where(
            quad == 1, pltpu.roll(edge, 1, 1), pltpu.roll(edge, lanes - 1, 1)
        )

    def x_line(field, value, edge, edge_in):
        turn = (lanes - 2 - 4 * field) % lanes
        two = pltpu.roll(edge, turn, 1)
        one = pltpu.roll(edge_in, turn, 1)
        m2 = jnp.where(edge_two & (lane < 64), two, pltpu.roll(value, 2, 1))
        m1 = jnp.where(edge_one & (lane < 64), one, pltpu.roll(value, 1, 1))
        p1 = jnp.where(edge_one & (lane >= 64), one, pltpu.roll(value, lanes - 1, 1))
        p2 = jnp.where(edge_two & (lane >= 64), two, pltpu.roll(value, lanes - 2, 1))
        return m2, m1, p1, p2

    def y_line(read):
        return tuple(read(0, dy) for dy in (-2, -1, 1, 2))

    def z_line(read):
        return tuple(read(dz, 0) for dz in (-2, -1, 1, 2))

    edge = strip()
    edge_in = inner(edge)
    edge_y = first_of(*y_line(strip))
    edge_y_in = inner(edge_y)
    edge_z = first_of(*z_line(strip))
    edge_z_in = inner(edge_z)

    centre, grad, curve, lap, mixed = {}, {}, {}, {}, {}
    need_lap = (0, 1, 2, 3, 4, 5, 6, 17, 18, 19, 20)
    shift = [cell(18), cell(19), cell(20)]
    advected = {}
    for field in range(len(ORDER)):
        centre[field] = cell(field)

    def differentiate(field):
        value = centre[field]
        read = functools.partial(cell, field)
        lines = [x_line(field, value, edge, edge_in), y_line(read), z_line(read)]
        near = [m1 + p1 for _, m1, p1, _ in lines]
        far = [m2 + p2 for m2, _, _, p2 in lines]
        near_sum = near[0] + near[1] + near[2]
        far_sum = far[0] + far[1] + far[2]
        smooth = far_sum - 4.0 * near_sum + 18.0 * value
        grads = [first_of(*line) for line in lines]
        grad[field] = grads
        advected[field] = (
            shift[0] * grads[0] + shift[1] * grads[1] + shift[2] * grads[2]
            - (DISSIPATE / 16.0) * smooth
        )
        if field in need_lap:
            lap[field] = (16.0 / 12.0) * near_sum - (1.0 / 12.0) * far_sum - 7.5 * value
        if field in MIXED:
            for axis in range(3):
                if field in (0, 17) or field == 18 + axis:
                    curve[field, axis] = (
                        (16.0 / 12.0) * near[axis] - (1.0 / 12.0) * far[axis] - 2.5 * value
                    )
            if field != 20:
                mixed[field, 0, 1] = first_of(*x_line(field, grads[1], edge_y, edge_y_in))
            if field != 19:
                mixed[field, 0, 2] = first_of(*x_line(field, grads[2], edge_z, edge_z_in))
            if field != 18:
                mixed[field, 1, 2] = first_of(
                    *(
                        first_of(*(cell(field, dz, dy) for dy in (-2, -1, 1, 2)))
                        for dz in (-2, -1, 1, 2)
                    )
                )

    def second(field, one, two):
        if one == two:
            return curve[field, one]
        return mixed[field, min(one, two), max(one, two)]

    def sym(table, one, two):
        return table[PAIR_SLOT[one][two]]

    metric = [centre[1 + k] for k in range(6)]
    traceless = [centre[8 + k] for k in range(6)]
    inverse = [
        (2.0 - metric[k]) if one == two else -metric[k]
        for k, (one, two) in enumerate(PAIR_LIST)
    ]

    def contract(left, right):
        diag = left[0] * right[0] + left[3] * right[3] + left[5] * right[5]
        off = left[1] * right[1] + left[2] * right[2] + left[4] * right[4]
        return diag + 2.0 * off

    def lie_of(table, one, two):
        total = None
        for k in range(3):
            if one == two:
                term = 2.0 * (sym(table, one, k) * grad[18 + k][one])
            else:
                term = (
                    sym(table, one, k) * grad[18 + k][two]
                    + sym(table, two, k) * grad[18 + k][one]
                )
            total = term if total is None else total + term
        return total

    group = len(ORDER) // GROUPS

    def begin(stage):
        for field in ORDER[stage * group : (stage + 1) * group]:
            differentiate(field)

    chi, trace, lapse, theta = centre[0], centre[7], centre[17], centre[24]

    begin(0)
    div = grad[18][0] + grad[19][1] + grad[20][2]
    third_div = (2.0 / 3.0) * div
    emit(0, advected[0] + (2.0 / 3.0) * chi * (lapse * trace) - chi * third_div)
    emit(17, advected[17] - 2.0 * lapse * (trace - 2.0 * theta))
    for one in range(3):
        emit(18 + one, advected[18 + one] + 0.75 * centre[21 + one])
    yield

    def metric_rate(k):
        one, two = PAIR_LIST[k]
        emit(
            1 + k,
            advected[1 + k]
            - 2.0 * lapse * traceless[k]
            + lie_of(metric, one, two)
            - metric[k] * third_div,
        )

    begin(1)
    for k in range(5):
        metric_rate(k)
    yield

    begin(2)
    metric_rate(5)
    over_chi = 1.0 / chi
    half_over = 0.5 * over_chi
    squares = contract(traceless, traceless)
    lapse_dd = [second(17, one, two) for one, two in PAIR_LIST]
    lapse_trace = contract(inverse, lapse_dd)
    emit(
        7,
        advected[7]
        - chi * lapse_trace
        + lapse * (squares + trace * trace * (1.0 / 3.0))
        + KAPPA_ONE * lapse * theta,
    )
    gauges = []
    for one in range(3):
        a_lapse = sum(sym(traceless, one, k) * grad[17][k] for k in range(3))
        a_chi = sum(sym(traceless, one, k) * grad[0][k] for k in range(3))
        g_trace = sum(sym(inverse, one, k) * grad[7][k] for k in range(3))
        b_mixed = sum(second(18 + k, one, k) for k in range(3))
        g_shift = sum(centre[14 + k] * grad[18 + one][k] for k in range(3))
        gauge = (
            -2.0 * a_lapse
            - lapse * ((4.0 / 3.0) * g_trace + 3.0 * (a_chi * over_chi))
            + lap[18 + one]
            + b_mixed * (1.0 / 3.0)
            + centre[14 + one] * third_div
            - g_shift
        )
        gauges.append(gauge)
        emit(14 + one, advected[14 + one] + gauge)
    yield

    begin(3)
    ricci = []
    for k, (one, two) in enumerate(PAIR_LIST):
        conf = second(0, one, two)
        if one == two:
            conf = conf + lap[0]
            grads_g = grad[14 + one][one]
        else:
            grads_g = 0.5 * (grad[14 + two][one] + grad[14 + one][two])
        ricci.append(-0.5 * lap[1 + k] + grads_g + conf * half_over)
    ricci_trace = contract(inverse, ricci)
    third_trace = (lapse * ricci_trace - lapse_trace) * (1.0 / 3.0)

    def traceless_rate(k):
        one, two = PAIR_LIST[k]
        free = lapse * ricci[k] - lapse_dd[k] - metric[k] * third_trace
        product = sum(
            sym(traceless, one, m) * sym(traceless, m, two) for m in range(3)
        )
        emit(
            8 + k,
            advected[8 + k]
            + chi * free
            + lapse * (trace * traceless[k] - 2.0 * product)
            + lie_of(traceless, one, two)
            - traceless[k] * third_div,
        )

    for k in range(5):
        traceless_rate(k)
    yield

    begin(4)
    traceless_rate(5)
    for one in range(3):
        emit(21 + one, advected[21 + one] + gauges[one] - DRIVER_ETA * centre[21 + one])
    emit(
        24,
        advected[24]
        + 0.5 * lapse * (chi * ricci_trace + (2.0 / 3.0) * trace * trace - squares)
        - 2.0 * KAPPA_ONE * lapse * theta,
    )
    yield


def section_kernel(
    sizes, groups, section, base, accum, ns_out, na_out, slab,
    xb, tb, tile, bb, ab, local_sem, halo_send, halo_recv,
    line_send, gather_recv,
):
    gx, gy, gz = sizes
    fields, planes, rows, lanes = section.shape
    i, j, k = (lax.axis_index(name) for name in ("gx", "gy", "gz"))
    group = fields // groups

    def device(dx=0, dy=0, dz=0):
        return (
            lax.rem(i + dx + gx, gx),
            lax.rem(j + dy + gy, gy),
            lax.rem(k + dz + gz, gz),
        )

    x_steps = (1,) if gx == 2 else (1, -1)
    messages = []

    def plane_pair(dz):
        if dz == 0:
            return slice(0, planes), slice(2, 2 + planes)
        if dz == 1:
            return slice(planes - 2, planes), slice(0, 2)
        return slice(0, 2), slice(2 + planes, 4 + planes)

    def row_pair(dy):
        if dy == 0:
            return slice(0, rows), slice(PAD, PAD + rows)
        if dy == 1:
            return slice(rows - 2, rows), slice(PAD - 2, PAD)
        return slice(0, 2), slice(PAD + rows, PAD + rows + 2)

    def at(ref, lead, plane_cut, row_cut):
        def ds(cut):
            return pl.ds(cut.start, cut.stop - cut.start)

        return ref.at[lead, ds(plane_cut), ds(row_cut), :]

    def own(cut_p, cut_r):
        return (
            slice(cut_p.start + 2, cut_p.stop + 2),
            slice(cut_r.start + PAD, cut_r.stop + PAD),
        )

    stages = [[] for _ in range(groups)]

    def add(stage, delta, src, dst):
        stages[stage].append(len(messages))
        messages.append((delta, src, dst))

    def face(stage, delta):
        src_p, dst_p = plane_pair(delta[2])
        src_r, dst_r = row_pair(delta[1])
        run = pl.ds(stage * group, group)
        add(stage, delta, at(xb, run, *own(src_p, src_r)), at(xb, run, dst_p, dst_r))

    for stage in range(groups):
        for step in (1, -1):
            face(stage, (0, step, 0))
            face(stage, (0, 0, step))
        if stage == 0:
            for dy in (1, -1):
                for dz in (1, -1):
                    face(0, (0, dy, dz))
    direct = len(messages)
    for slot, dx in enumerate(x_steps):
        for dy, dz in ((0, 0), (1, 0), (-1, 0), (0, 1), (0, -1)):
            src_p, dst_p = plane_pair(dz)
            src_r, dst_r = row_pair(dy)
            add(0, (dx, dy, dz), at(tile, 0, src_p, src_r), at(tb, slot, dst_p, dst_r))

    loads = []
    place = 0
    for first, size in RUNS:
        loads.append(
            pltpu.make_async_copy(
                section.at[pl.ds(first, size)],
                xb.at[pl.ds(place, size), pl.ds(2, planes), pl.ds(PAD, rows), :],
                local_sem.at[2 + len(loads)],
            )
        )
        place += size
    load_base = pltpu.make_async_copy(base, bb, local_sem.at[0])
    load_accum = pltpu.make_async_copy(accum, ab, local_sem.at[1])
    for load in loads:
        load.start()
    load_base.start()
    load_accum.start()

    partners = []
    for delta, _, _ in messages:
        if delta not in partners:
            partners.append(delta)
    barrier = pltpu.get_barrier_semaphore()
    for delta in partners:
        pl.semaphore_signal(barrier, inc=1, device_id=device(*delta), device_id_type=MESH)
    pl.semaphore_wait(barrier, len(partners))

    copies = [
        pltpu.make_async_remote_copy(
            src_ref=src, dst_ref=dst, send_sem=halo_send.at[m], recv_sem=halo_recv.at[m],
            device_id=device(*delta), device_id_type=MESH,
        )
        for m, (delta, src, dst) in enumerate(messages)
    ]
    for load in loads:
        load.wait()
    for copy in copies[:direct]:
        copy.start()
    lane = lax.broadcasted_iota(jnp.int32, (rows, lanes), 1)

    def pack(plane, carry):
        packed = jnp.zeros((rows, lanes), jnp.float32)
        for field in range(fields):
            value = xb[PLACE[field], plane + 2, PAD : PAD + rows, :]
            ends = jnp.where(lane < 2, value, pltpu.roll(value, 4, 1))
            if field:
                ends = pltpu.roll(ends, 4 * field, 1)
            packed = jnp.where((lane >> 2) == field, ends, packed)
        tile[0, plane] = packed
        return carry

    lax.fori_loop(0, planes, pack, 0)
    for copy in copies[direct:]:
        copy.start()
    load_base.wait()
    load_accum.wait()

    own_rows = pl.ds(pl.multiple_of(j * rows, rows), rows)
    own_cols = pl.ds(pl.multiple_of(i * lanes, lanes), lanes)

    def piece(ref, bi, bj, c=None):
        lead = pl.ds(0, fields) if c is None else pl.ds(c * group, group)
        return ref.at[
            lead,
            :,
            pl.ds(pl.multiple_of(bj * rows, rows), rows),
            pl.ds(pl.multiple_of(bi * lanes, lanes), lanes),
        ]

    towards = ((0, 1), (0, -1), (1, 0), (-1, 0))

    def send(link, bi, bj, c):
        dx, dy = towards[link]
        return pltpu.make_async_remote_copy(
            src_ref=piece(slab, bi, bj, c),
            dst_ref=piece(slab, bi, bj, c),
            send_sem=line_send.at[link, bi, bj, c],
            recv_sem=gather_recv.at[bi, bj, c],
            device_id=device(dx, dy, 0),
            device_id_type=MESH,
        )

    def arrive(bi, bj, c):
        part = piece(slab, bi, bj, c)
        pltpu.make_async_remote_copy(
            src_ref=part, dst_ref=part, send_sem=line_send.at[0, bi, bj, c],
            recv_sem=gather_recv.at[bi, bj, c], device_id=device(0, 1, 0),
            device_id_type=MESH,
        ).wait_recv()

    paired = gx == 2 and gy % 2 == 0
    turned = (groups * 2) // 5 if paired else 0
    pair = j + 1 - 2 * lax.rem(j, 2)

    def each(count, body, start=0):
        lax.fori_loop(start, count, lambda c, carry: (body(c), carry)[1], 0)

    def x_links(body):
        @pl.when(i + 1 < gx)
        def _():
            body(2)

        @pl.when(i > 0)
        def _():
            body(3)

    def send_own(c):
        @pl.when(j + 1 < gy)
        def _():
            send(0, i, j, c).start()

        @pl.when(j > 0)
        def _():
            send(1, i, j, c).start()

        x_links(lambda link: send(link, i, j, c).start())

    def emit_at(plane):
        def emit(field, rate):
            moved = bb[field, plane] + (0.5 * STEP_DT) * rate
            slab[PLACE[field], plane, own_rows, own_cols] = moved
            ns_out[field, plane] = moved
            na_out[field, plane] = ab[field, plane] + (STEP_DT / 3.0) * rate

        return emit

    def await_rows(stage, along_y):
        for m in stages[stage]:
            if (messages[m][0][2] == 0) == along_y:
                copies[m].wait_recv()

    await_rows(0, True)
    await_rows(0, False)
    work = [
        rates_of_plane(plane, rows, lanes, xb, tb, emit_at(plane))
        for plane in range(planes)
    ]
    for stage in range(groups):
        for part in work:
            next(part)
        if stage + 1 < groups:
            await_rows(stage + 1, True)
        send_own(stage)
        if stage + 1 < groups:
            await_rows(stage + 1, False)

    def crossed(d, bj, c, body):
        if d == 1 and turned:
            @pl.when((bj != pair) | (c >= turned))
            def _():
                body()
        else:
            body()

    other = 1 - i

    for d in range(1, gy):
        def column(c, d=d):
            @pl.when(j - d >= 0)
            def _():
                bj = j - d
                arrive(i, bj, c)

                @pl.when(j + 1 < gy)
                def _():
                    send(0, i, bj, c).start()

                crossed(d, bj, c, lambda: x_links(lambda link: send(link, i, bj, c).start()))

            @pl.when(j + d < gy)
            def _():
                bj = j + d
                arrive(i, bj, c)

                @pl.when(j > 0)
                def _():
                    send(1, i, bj, c).start()

                crossed(d, bj, c, lambda: x_links(lambda link: send(link, i, bj, c).start()))

            if d == 1 and turned:
                @pl.when(c < turned)
                def _():
                    arrive(other, j, c)

                    @pl.when(pair > j)
                    def _():
                        send(0, other, j, c).start()

                    @pl.when(pair < j)
                    def _():
                        send(1, other, j, c).start()

        each(groups, column)

        @pl.when(j - d >= 0)
        def _():
            pass

        @pl.when(j + d < gy)
        def _():
            pass

    def block_rows(body):
        body(j, True)
        for d in range(1, gy):
            @pl.when(j - d >= 0)
            def _():
                body(j - d, False)

            @pl.when(j + d < gy)
            def _():
                body(j + d, False)

    for d in range(1, gx):
        def row(bj, first, d=d):
            @pl.when(i - d >= 0)
            def _():
                def take(c):
                    arrive(i - d, bj, c)

                    @pl.when(i + 1 < gx)
                    def _():
                        send(2, i - d, bj, c).start()

                each(groups, take, turned if first else 0)
                pass

            @pl.when(i + d < gx)
            def _():
                def take(c):
                    arrive(i + d, bj, c)

                    @pl.when(i > 0)
                    def _():
                        send(3, i + d, bj, c).start()

                each(groups, take, turned if first else 0)
                pass

        block_rows(row)

    for copy in copies:
        copy.wait_send()

    def drain(bj):
        def chunk(c):
            @pl.when((bj <= j) & (j + 1 < gy))
            def _():
                send(0, i, bj, c).wait_send()

            @pl.when((bj >= j) & (j > 0))
            def _():
                send(1, i, bj, c).wait_send()

            def sideways(link):
                send(link, i, bj, c).wait_send()

            if turned:
                @pl.when((bj != pair) | (c >= turned))
                def _():
                    x_links(sideways)
            else:
                x_links(sideways)

            for d in range(1, gx):
                @pl.when((i - d >= 0) & (i + 1 < gx))
                def _():
                    send(2, i - d, bj, c).wait_send()

                @pl.when((i + d < gx) & (i > 0))
                def _():
                    send(3, i + d, bj, c).wait_send()

        each(groups, chunk)

    each(gy, drain)
    if turned:
        def drain_turned(c):
            @pl.when(pair > j)
            def _():
                send(0, other, j, c).wait_send()

            @pl.when(pair < j)
            def _():
                send(1, other, j, c).wait_send()

        each(turned, drain_turned)


def put_out(ns_in, na_in, slab_in, ns_out, na_out, slab_out, sem):
    pairs = []
    place = 0
    for first, size in RUNS:
        pairs.append((slab_in.at[pl.ds(place, size)], slab_out.at[pl.ds(first, size)]))
        place += size
    pairs += [(ns_in, ns_out), (na_in, na_out)]
    copies = [pltpu.make_async_copy(a, b, sem.at[n]) for n, (a, b) in enumerate(pairs)]
    for copy in copies:
        copy.start()
    for copy in copies:
        copy.wait()


def shards(sizes, section, base, accum):
    gx, gy, gz = sizes
    fields, planes, rows, lanes = section.shape
    groups = GROUPS
    slots = 1 if gx == 2 else 2
    n_messages = 4 * groups + 4 + 5 * slots
    any_spec = pl.BlockSpec(memory_space=pl.ANY)
    block = jax.ShapeDtypeStruct(section.shape, jnp.float32)
    slab = jax.ShapeDtypeStruct((fields, planes, gy * rows, gx * lanes), jnp.float32)
    dma = pltpu.SemaphoreType.DMA
    staged = pl.pallas_call(
        functools.partial(section_kernel, sizes, groups),
        out_shape=tuple(pltpu.VMEM(a.shape, a.dtype) for a in (block, block, slab)),
        in_specs=[pl.BlockSpec(memory_space=pltpu.HBM)] * 3,
        out_specs=(pl.BlockSpec(memory_space=pltpu.VMEM),) * 3,
        scratch_shapes=[
            pltpu.VMEM((fields, planes + 4, rows + 2 * PAD, lanes), jnp.float32),
            pltpu.VMEM((slots, planes + 4, rows + 2 * PAD, lanes), jnp.float32),
            pltpu.VMEM((1, planes, rows, lanes), jnp.float32),
            pltpu.VMEM(section.shape, jnp.float32),
            pltpu.VMEM(section.shape, jnp.float32),
            dma((2 + len(RUNS),)),
            dma((n_messages,)),
            dma((n_messages,)),
            dma((4, gx, gy, groups)),
            dma((gx, gy, groups)),
        ],
        compiler_params=pltpu.CompilerParams(collective_id=0, has_side_effects=True, vmem_limit_bytes=24 << 20),
    )(*(pltpu.with_memory_space_constraint(x, pltpu.HBM) for x in (section, base, accum)))
    return pl.pallas_call(
        put_out,
        out_shape=(block, block, slab),
        in_specs=[pl.BlockSpec(memory_space=pltpu.VMEM)] * 3,
        out_specs=(any_spec,) * 3,
        scratch_shapes=[dma((2 + len(RUNS),))],
        compiler_params=pltpu.CompilerParams(vmem_limit_bytes=8 << 20),
    )(*staged)


def solution(mesh):
    sizes = tuple(mesh.shape[name] for name in ("gx", "gy", "gz"))
    spec = P(None, "gz", "gy", "gx")
    return jax.shard_map(
        functools.partial(shards, sizes),
        mesh=mesh,
        in_specs=(spec, spec, spec),
        out_specs=(spec, spec, P(None, "gz", None, None)),
        check_vma=False,
    )
```

```python
import functools

import jax
import jax.numpy as jnp
from jax import lax
from jax.experimental import pallas as pl
from jax.experimental.pallas import tpu as pltpu
from jax.sharding import PartitionSpec as P

STEP_DT = 0.25
DISSIPATE = 0.1
DRIVER_ETA = 2.0
KAPPA_ONE = 0.1
PAIR_SLOT = ((0, 1, 2), (1, 3, 4), (2, 4, 5))
PAIR_LIST = ((0, 0), (0, 1), (0, 2), (1, 1), (1, 2), (2, 2))
MESH = pl.DeviceIdType.MESH
MIXED = (0, 17, 18, 19, 20)
RUNS = ((0, 1), (17, 4), (1, 5), (6, 2), (14, 3), (8, 5), (13, 1), (21, 4))
GROUPS = 5
ORDER = tuple(first + n for first, size in RUNS for n in range(size))
PLACE = tuple(ORDER.index(field) for field in range(len(ORDER)))
PAD = 8


def first_of(m2, m1, p1, p2):
    return (8.0 / 12.0) * (p1 - m1) - (1.0 / 12.0) * (p2 - m2)


def rates_of_plane(plane, rows, lanes, xb, tb, emit):
    lane = lax.broadcasted_iota(jnp.int32, (rows, lanes), 1)
    quad = lane & 3
    edge_one = (lane < 1) | (lane >= lanes - 1)
    edge_two = (lane < 2) | (lane >= lanes - 2)

    def cell(field, dz=0, dy=0):
        return xb[PLACE[field], plane + 2 + dz, PAD + dy : PAD + dy + rows, :]

    def strip(dz=0, dy=0):
        def side(slot):
            return tb[slot, plane + 2 + dz, PAD + dy : PAD + dy + rows, :]

        if tb.shape[0] == 1:
            return side(0)
        return jnp.where(quad < 2, side(1), side(0))

    def inner(edge):
        return jnp.where(
            quad == 1, pltpu.roll(edge, 1, 1), pltpu.roll(edge, lanes - 1, 1)
        )

    def x_line(field, value, edge, edge_in):
        turn = (lanes - 2 - 4 * field) % lanes
        two = pltpu.roll(edge, turn, 1)
        one = pltpu.roll(edge_in, turn, 1)
        m2 = jnp.where(edge_two & (lane < 64), two, pltpu.roll(value, 2, 1))
        m1 = jnp.where(edge_one & (lane < 64), one, pltpu.roll(value, 1, 1))
        p1 = jnp.where(edge_one & (lane >= 64), one, pltpu.roll(value, lanes - 1, 1))
        p2 = jnp.where(edge_two & (lane >= 64), two, pltpu.roll(value, lanes - 2, 1))
        return m2, m1, p1, p2

    def y_line(read):
        return tuple(read(0, dy) for dy in (-2, -1, 1, 2))

    def z_line(read):
        return tuple(read(dz, 0) for dz in (-2, -1, 1, 2))

    edge = strip()
    edge_in = inner(edge)
    edge_y = first_of(*y_line(strip))
    edge_y_in = inner(edge_y)
    edge_z = first_of(*z_line(strip))
    edge_z_in = inner(edge_z)

    centre, grad, curve, lap, mixed = {}, {}, {}, {}, {}
    need_lap = (0, 1, 2, 3, 4, 5, 6, 17, 18, 19, 20)
    shift = [cell(18), cell(19), cell(20)]
    advected = {}
    for field in range(len(ORDER)):
        centre[field] = cell(field)

    def differentiate(field):
        value = centre[field]
        read = functools.partial(cell, field)
        lines = [x_line(field, value, edge, edge_in), y_line(read), z_line(read)]
        near = [m1 + p1 for _, m1, p1, _ in lines]
        far = [m2 + p2 for m2, _, _, p2 in lines]
        near_sum = near[0] + near[1] + near[2]
        far_sum = far[0] + far[1] + far[2]
        smooth = far_sum - 4.0 * near_sum + 18.0 * value
        grads = [first_of(*line) for line in lines]
        grad[field] = grads
        advected[field] = (
            shift[0] * grads[0] + shift[1] * grads[1] + shift[2] * grads[2]
            - (DISSIPATE / 16.0) * smooth
        )
        if field in need_lap:
            lap[field] = (16.0 / 12.0) * near_sum - (1.0 / 12.0) * far_sum - 7.5 * value
        if field in MIXED:
            for axis in range(3):
                if field in (0, 17) or field == 18 + axis:
                    curve[field, axis] = (
                        (16.0 / 12.0) * near[axis] - (1.0 / 12.0) * far[axis] - 2.5 * value
                    )
            if field != 20:
                mixed[field, 0, 1] = first_of(*x_line(field, grads[1], edge_y, edge_y_in))
            if field != 19:
                mixed[field, 0, 2] = first_of(*x_line(field, grads[2], edge_z, edge_z_in))
            if field != 18:
                mixed[field, 1, 2] = first_of(
                    *(
                        first_of(*(cell(field, dz, dy) for dy in (-2, -1, 1, 2)))
                        for dz in (-2, -1, 1, 2)
                    )
                )

    def second(field, one, two):
        if one == two:
            return curve[field, one]
        return mixed[field, min(one, two), max(one, two)]

    def sym(table, one, two):
        return table[PAIR_SLOT[one][two]]

    metric = [centre[1 + k] for k in range(6)]
    traceless = [centre[8 + k] for k in range(6)]
    inverse = [
        (2.0 - metric[k]) if one == two else -metric[k]
        for k, (one, two) in enumerate(PAIR_LIST)
    ]

    def contract(left, right):
        diag = left[0] * right[0] + left[3] * right[3] + left[5] * right[5]
        off = left[1] * right[1] + left[2] * right[2] + left[4] * right[4]
        return diag + 2.0 * off

    def lie_of(table, one, two):
        total = None
        for k in range(3):
            if one == two:
                term = 2.0 * (sym(table, one, k) * grad[18 + k][one])
            else:
                term = (
                    sym(table, one, k) * grad[18 + k][two]
                    + sym(table, two, k) * grad[18 + k][one]
                )
            total = term if total is None else total + term
        return total

    group = len(ORDER) // GROUPS

    def begin(stage):
        for field in ORDER[stage * group : (stage + 1) * group]:
            differentiate(field)

    chi, trace, lapse, theta = centre[0], centre[7], centre[17], centre[24]

    begin(0)
    div = grad[18][0] + grad[19][1] + grad[20][2]
    third_div = (2.0 / 3.0) * div
    emit(0, advected[0] + (2.0 / 3.0) * chi * (lapse * trace) - chi * third_div)
    emit(17, advected[17] - 2.0 * lapse * (trace - 2.0 * theta))
    for one in range(3):
        emit(18 + one, advected[18 + one] + 0.75 * centre[21 + one])
    yield

    def metric_rate(k):
        one, two = PAIR_LIST[k]
        emit(
            1 + k,
            advected[1 + k]
            - 2.0 * lapse * traceless[k]
            + lie_of(metric, one, two)
            - metric[k] * third_div,
        )

    begin(1)
    for k in range(5):
        metric_rate(k)
    yield

    begin(2)
    metric_rate(5)
    over_chi = 1.0 / chi
    half_over = 0.5 * over_chi
    squares = contract(traceless, traceless)
    lapse_dd = [second(17, one, two) for one, two in PAIR_LIST]
    lapse_trace = contract(inverse, lapse_dd)
    emit(
        7,
        advected[7]
        - chi * lapse_trace
        + lapse * (squares + trace * trace * (1.0 / 3.0))
        + KAPPA_ONE * lapse * theta,
    )
    gauges = []
    for one in range(3):
        a_lapse = sum(sym(traceless, one, k) * grad[17][k] for k in range(3))
        a_chi = sum(sym(traceless, one, k) * grad[0][k] for k in range(3))
        g_trace = sum(sym(inverse, one, k) * grad[7][k] for k in range(3))
        b_mixed = sum(second(18 + k, one, k) for k in range(3))
        g_shift = sum(centre[14 + k] * grad[18 + one][k] for k in range(3))
        gauge = (
            -2.0 * a_lapse
            - lapse * ((4.0 / 3.0) * g_trace + 3.0 * (a_chi * over_chi))
            + lap[18 + one]
            + b_mixed * (1.0 / 3.0)
            + centre[14 + one] * third_div
            - g_shift
        )
        gauges.append(gauge)
        emit(14 + one, advected[14 + one] + gauge)
    yield

    begin(3)
    ricci = []
    for k, (one, two) in enumerate(PAIR_LIST):
        conf = second(0, one, two)
        if one == two:
            conf = conf + lap[0]
            grads_g = grad[14 + one][one]
        else:
            grads_g = 0.5 * (grad[14 + two][one] + grad[14 + one][two])
        ricci.append(-0.5 * lap[1 + k] + grads_g + conf * half_over)
    ricci_trace = contract(inverse, ricci)
    third_trace = (lapse * ricci_trace - lapse_trace) * (1.0 / 3.0)

    def traceless_rate(k):
        one, two = PAIR_LIST[k]
        free = lapse * ricci[k] - lapse_dd[k] - metric[k] * third_trace
        product = sum(
            sym(traceless, one, m) * sym(traceless, m, two) for m in range(3)
        )
        emit(
            8 + k,
            advected[8 + k]
            + chi * free
            + lapse * (trace * traceless[k] - 2.0 * product)
            + lie_of(traceless, one, two)
            - traceless[k] * third_div,
        )

    for k in range(5):
        traceless_rate(k)
    yield

    begin(4)
    traceless_rate(5)
    for one in range(3):
        emit(21 + one, advected[21 + one] + gauges[one] - DRIVER_ETA * centre[21 + one])
    emit(
        24,
        advected[24]
        + 0.5 * lapse * (chi * ricci_trace + (2.0 / 3.0) * trace * trace - squares)
        - 2.0 * KAPPA_ONE * lapse * theta,
    )
    yield


def section_kernel(
    sizes, groups, section, base, accum, ns_out, na_out, slab,
    xb, tb, tile, bb, ab, local_sem, halo_send, halo_recv,
    line_send, gather_recv,
):
    gx, gy, gz = sizes
    fields, planes, rows, lanes = section.shape
    i, j, k = (lax.axis_index(name) for name in ("gx", "gy", "gz"))
    group = fields // groups

    def device(dx=0, dy=0, dz=0):
        return (
            lax.rem(i + dx + gx, gx),
            lax.rem(j + dy + gy, gy),
            lax.rem(k + dz + gz, gz),
        )

    x_steps = (1,) if gx == 2 else (1, -1)
    messages = []

    def plane_pair(dz):
        if dz == 0:
            return slice(0, planes), slice(2, 2 + planes)
        if dz == 1:
            return slice(planes - 2, planes), slice(0, 2)
        return slice(0, 2), slice(2 + planes, 4 + planes)

    def row_pair(dy):
        if dy == 0:
            return slice(0, rows), slice(PAD, PAD + rows)
        if dy == 1:
            return slice(rows - 2, rows), slice(PAD - 2, PAD)
        return slice(0, 2), slice(PAD + rows, PAD + rows + 2)

    def at(ref, lead, plane_cut, row_cut):
        def ds(cut):
            return pl.ds(cut.start, cut.stop - cut.start)

        return ref.at[lead, ds(plane_cut), ds(row_cut), :]

    def own(cut_p, cut_r):
        return (
            slice(cut_p.start + 2, cut_p.stop + 2),
            slice(cut_r.start + PAD, cut_r.stop + PAD),
        )

    stages = [[] for _ in range(groups)]

    def add(stage, delta, src, dst):
        stages[stage].append(len(messages))
        messages.append((delta, src, dst))

    def face(stage, delta):
        src_p, dst_p = plane_pair(delta[2])
        src_r, dst_r = row_pair(delta[1])
        run = pl.ds(stage * group, group)
        add(stage, delta, at(xb, run, *own(src_p, src_r)), at(xb, run, dst_p, dst_r))

    for stage in range(groups):
        for step in (1, -1):
            face(stage, (0, step, 0))
            face(stage, (0, 0, step))
        if stage == 0:
            for dy in (1, -1):
                for dz in (1, -1):
                    face(0, (0, dy, dz))
    direct = len(messages)
    for slot, dx in enumerate(x_steps):
        for dy, dz in ((0, 0), (1, 0), (-1, 0), (0, 1), (0, -1)):
            src_p, dst_p = plane_pair(dz)
            src_r, dst_r = row_pair(dy)
            add(0, (dx, dy, dz), at(tile, 0, src_p, src_r), at(tb, slot, dst_p, dst_r))

    loads = []
    place = 0
    for first, size in RUNS:
        loads.append(
            pltpu.make_async_copy(
                section.at[pl.ds(first, size)],
                xb.at[pl.ds(place, size), pl.ds(2, planes), pl.ds(PAD, rows), :],
                local_sem.at[2 + len(loads)],
            )
        )
        place += size
    load_base = pltpu.make_async_copy(base, bb, local_sem.at[0])
    load_accum = pltpu.make_async_copy(accum, ab, local_sem.at[1])
    for load in loads:
        load.start()
    load_base.start()
    load_accum.start()

    partners = []
    for delta, _, _ in messages:
        if delta not in partners:
            partners.append(delta)
    barrier = pltpu.get_barrier_semaphore()
    for delta in partners:
        pl.semaphore_signal(barrier, inc=1, device_id=device(*delta), device_id_type=MESH)

    copies = [
        pltpu.make_async_remote_copy(
            src_ref=src, dst_ref=dst, send_sem=halo_send.at[m], recv_sem=halo_recv.at[m],
            device_id=device(*delta), device_id_type=MESH,
        )
        for m, (delta, src, dst) in enumerate(messages)
    ]
    for load in loads:
        load.wait()
    lane = lax.broadcasted_iota(jnp.int32, (rows, lanes), 1)

    def pack(plane, carry):
        packed = jnp.zeros((rows, lanes), jnp.float32)
        for field in range(fields):
            value = xb[PLACE[field], plane + 2, PAD : PAD + rows, :]
            ends = jnp.where(lane < 2, value, pltpu.roll(value, 4, 1))
            if field:
                ends = pltpu.roll(ends, 4 * field, 1)
            packed = jnp.where((lane >> 2) == field, ends, packed)
        tile[0, plane] = packed
        return carry

    lax.fori_loop(0, planes, pack, 0)
    pl.semaphore_wait(barrier, len(partners))
    def block(m):
        return messages[m][0][:2] == (0, 0)

    order = sorted(range(len(messages)), key=lambda m: (block(m), m < direct))
    for m in order:
        copies[m].start()
    load_base.wait()
    load_accum.wait()

    own_rows = pl.ds(pl.multiple_of(j * rows, rows), rows)
    own_cols = pl.ds(pl.multiple_of(i * lanes, lanes), lanes)

    def piece(ref, bi, bj, c=None):
        lead = pl.ds(0, fields) if c is None else pl.ds(c * group, group)
        return ref.at[
            lead,
            :,
            pl.ds(pl.multiple_of(bj * rows, rows), rows),
            pl.ds(pl.multiple_of(bi * lanes, lanes), lanes),
        ]

    towards = ((0, 1), (0, -1), (1, 0), (-1, 0))

    def send(link, bi, bj, c):
        dx, dy = towards[link]
        return pltpu.make_async_remote_copy(
            src_ref=piece(slab, bi, bj, c),
            dst_ref=piece(slab, bi, bj, c),
            send_sem=line_send.at[link, bi, bj, c],
            recv_sem=gather_recv.at[bi, bj, c],
            device_id=device(dx, dy, 0),
            device_id_type=MESH,
        )

    def arrive(bi, bj, c):
        part = piece(slab, bi, bj, c)
        pltpu.make_async_remote_copy(
            src_ref=part, dst_ref=part, send_sem=line_send.at[0, bi, bj, c],
            recv_sem=gather_recv.at[bi, bj, c], device_id=device(0, 1, 0),
            device_id_type=MESH,
        ).wait_recv()

    paired = gx == 2 and gy % 2 == 0
    turned = (groups * 2) // 5 if paired else 0
    pair = j + 1 - 2 * lax.rem(j, 2)

    def each(count, body, start=0):
        lax.fori_loop(start, count, lambda c, carry: (body(c), carry)[1], 0)

    def x_links(body):
        @pl.when(i + 1 < gx)
        def _():
            body(2)

        @pl.when(i > 0)
        def _():
            body(3)

    def send_own(c):
        @pl.when(j + 1 < gy)
        def _():
            send(0, i, j, c).start()

        @pl.when(j > 0)
        def _():
            send(1, i, j, c).start()

        x_links(lambda link: send(link, i, j, c).start())

    def emit_at(plane):
        def emit(field, rate):
            moved = bb[field, plane] + (0.5 * STEP_DT) * rate
            slab[PLACE[field], plane, own_rows, own_cols] = moved
            ns_out[field, plane] = moved
            na_out[field, plane] = ab[field, plane] + (STEP_DT / 3.0) * rate

        return emit

    def await_rows(stage, along_y):
        for m in stages[stage]:
            if (messages[m][0][2] == 0) == along_y:
                copies[m].wait_recv()

    await_rows(0, True)
    await_rows(0, False)
    work = [
        rates_of_plane(plane, rows, lanes, xb, tb, emit_at(plane))
        for plane in range(planes)
    ]
    for stage in range(groups):
        for part in work:
            next(part)
        if stage + 1 < groups:
            await_rows(stage + 1, True)
        send_own(stage)
        if stage + 1 < groups:
            await_rows(stage + 1, False)

    def crossed(d, bj, c, body):
        if d == 1 and turned:
            @pl.when((bj != pair) | (c >= turned))
            def _():
                body()
        else:
            body()

    other = 1 - i

    for d in range(1, gy):
        def column(c, d=d):
            @pl.when(j - d >= 0)
            def _():
                bj = j - d
                arrive(i, bj, c)

                @pl.when(j + 1 < gy)
                def _():
                    send(0, i, bj, c).start()

                crossed(d, bj, c, lambda: x_links(lambda link: send(link, i, bj, c).start()))

            @pl.when(j + d < gy)
            def _():
                bj = j + d
                arrive(i, bj, c)

                @pl.when(j > 0)
                def _():
                    send(1, i, bj, c).start()

                crossed(d, bj, c, lambda: x_links(lambda link: send(link, i, bj, c).start()))

            if d == 1 and turned:
                @pl.when(c < turned)
                def _():
                    arrive(other, j, c)

                    @pl.when(pair > j)
                    def _():
                        send(0, other, j, c).start()

                    @pl.when(pair < j)
                    def _():
                        send(1, other, j, c).start()

        each(groups, column)

        @pl.when(j - d >= 0)
        def _():
            pass

        @pl.when(j + d < gy)
        def _():
            pass

    def block_rows(body):
        body(j, True)
        for d in range(1, gy):
            @pl.when(j - d >= 0)
            def _():
                body(j - d, False)

            @pl.when(j + d < gy)
            def _():
                body(j + d, False)

    for d in range(1, gx):
        def row(bj, first, d=d):
            @pl.when(i - d >= 0)
            def _():
                def take(c):
                    arrive(i - d, bj, c)

                    @pl.when(i + 1 < gx)
                    def _():
                        send(2, i - d, bj, c).start()

                each(groups, take, turned if first else 0)
                pass

            @pl.when(i + d < gx)
            def _():
                def take(c):
                    arrive(i + d, bj, c)

                    @pl.when(i > 0)
                    def _():
                        send(3, i + d, bj, c).start()

                each(groups, take, turned if first else 0)
                pass

        block_rows(row)

    for copy in copies:
        copy.wait_send()

    def drain(bj):
        def chunk(c):
            @pl.when((bj <= j) & (j + 1 < gy))
            def _():
                send(0, i, bj, c).wait_send()

            @pl.when((bj >= j) & (j > 0))
            def _():
                send(1, i, bj, c).wait_send()

            def sideways(link):
                send(link, i, bj, c).wait_send()

            if turned:
                @pl.when((bj != pair) | (c >= turned))
                def _():
                    x_links(sideways)
            else:
                x_links(sideways)

            for d in range(1, gx):
                @pl.when((i - d >= 0) & (i + 1 < gx))
                def _():
                    send(2, i - d, bj, c).wait_send()

                @pl.when((i + d < gx) & (i > 0))
                def _():
                    send(3, i + d, bj, c).wait_send()

        each(groups, chunk)

    each(gy, drain)
    if turned:
        def drain_turned(c):
            @pl.when(pair > j)
            def _():
                send(0, other, j, c).wait_send()

            @pl.when(pair < j)
            def _():
                send(1, other, j, c).wait_send()

        each(turned, drain_turned)


def put_out(ns_in, na_in, slab_in, ns_out, na_out, slab_out, sem):
    pairs = []
    place = 0
    for first, size in RUNS:
        pairs.append((slab_in.at[pl.ds(place, size)], slab_out.at[pl.ds(first, size)]))
        place += size
    pairs += [(ns_in, ns_out), (na_in, na_out)]
    copies = [pltpu.make_async_copy(a, b, sem.at[n]) for n, (a, b) in enumerate(pairs)]
    for copy in copies:
        copy.start()
    for copy in copies:
        copy.wait()


def shards(sizes, section, base, accum):
    gx, gy, gz = sizes
    fields, planes, rows, lanes = section.shape
    groups = GROUPS
    slots = 1 if gx == 2 else 2
    n_messages = 4 * groups + 4 + 5 * slots
    any_spec = pl.BlockSpec(memory_space=pl.ANY)
    block = jax.ShapeDtypeStruct(section.shape, jnp.float32)
    slab = jax.ShapeDtypeStruct((fields, planes, gy * rows, gx * lanes), jnp.float32)
    dma = pltpu.SemaphoreType.DMA
    staged = pl.pallas_call(
        functools.partial(section_kernel, sizes, groups),
        out_shape=tuple(pltpu.VMEM(a.shape, a.dtype) for a in (block, block, slab)),
        in_specs=[pl.BlockSpec(memory_space=pltpu.HBM)] * 3,
        out_specs=(pl.BlockSpec(memory_space=pltpu.VMEM),) * 3,
        scratch_shapes=[
            pltpu.VMEM((fields, planes + 4, rows + 2 * PAD, lanes), jnp.float32),
            pltpu.VMEM((slots, planes + 4, rows + 2 * PAD, lanes), jnp.float32),
            pltpu.VMEM((1, planes, rows, lanes), jnp.float32),
            pltpu.VMEM(section.shape, jnp.float32),
            pltpu.VMEM(section.shape, jnp.float32),
            dma((2 + len(RUNS),)),
            dma((n_messages,)),
            dma((n_messages,)),
            dma((4, gx, gy, groups)),
            dma((gx, gy, groups)),
        ],
        compiler_params=pltpu.CompilerParams(collective_id=0, has_side_effects=True, vmem_limit_bytes=24 << 20),
    )(*(pltpu.with_memory_space_constraint(x, pltpu.HBM) for x in (section, base, accum)))
    return pl.pallas_call(
        put_out,
        out_shape=(block, block, slab),
        in_specs=[pl.BlockSpec(memory_space=pltpu.VMEM)] * 3,
        out_specs=(any_spec,) * 3,
        scratch_shapes=[dma((2 + len(RUNS),))],
        compiler_params=pltpu.CompilerParams(vmem_limit_bytes=8 << 20),
    )(*staged)


def solution(mesh):
    sizes = tuple(mesh.shape[name] for name in ("gx", "gy", "gz"))
    spec = P(None, "gz", "gy", "gx")
    return jax.shard_map(
        functools.partial(shards, sizes),
        mesh=mesh,
        in_specs=(spec, spec, spec),
        out_specs=(spec, spec, P(None, "gz", None, None)),
        check_vma=False,
    )
```
